8 devices in a mesh: dp: 1 (over z), tp: 8 (over y, x, core).
Axes of the slice: x: 2, y: 2, z: 1, core: 2. Of those that a mesh axis runs over, the one named last changes fastest.
Arguments:
- x_norm: bfloat16 [4096, 4096], P(('dp', 'tp'))
- w_gate: bfloat16 [4096, 14336], P(None, 'tp')
- w_up: bfloat16 [4096, 14336], P(None, 'tp')
- w_down: bfloat16 [14336, 4096], P('tp')
- u_gate: bfloat16 [4096, 14336], P('dp', 'tp')
- u_up: bfloat16 [4096, 14336], P('dp', 'tp')
- grad_out: bfloat16 [4096, 4096], P(('dp', 'tp'))
Outputs:
- output 1: bfloat16 [4096, 4096], P(('dp', 'tp'))
- output 2: float32 [4096, 14336], P('dp', 'tp')
- output 3: float32 [4096, 14336], P('dp', 'tp')
- output 4: float32 [14336, 4096], P(('dp', 'tp'))
All inputs are finite; a program needn't handle non-finite values.
Results may differ from the reference program's by a relative error of at most 0.0104291.
Values are sent between devices in bfloat16 or wider.
A program may use at most 1 GiB of HBM per device.

```python
import jax
import jax.numpy as jnp
from jax import lax

HIDDEN = 4096
FFN_DIM = 14336
TOKENS = 4096
GROUP_SIZE = 8


def setup_inputs(seed: int = 0, part: int = 0) -> dict:
    base_key = jax.random.key(seed)
    w_keys = jax.random.split(base_key, 3)
    part_keys = jax.random.split(jax.random.fold_in(base_key, part), 4)
    w_gate = (jax.random.normal(w_keys[0], (HIDDEN, FFN_DIM), jnp.float32) * HIDDEN ** -0.5).astype(jnp.bfloat16)
    w_up = (jax.random.normal(w_keys[1], (HIDDEN, FFN_DIM), jnp.float32) * HIDDEN ** -0.5).astype(jnp.bfloat16)
    w_down = (jax.random.normal(w_keys[2], (FFN_DIM, HIDDEN), jnp.float32) * FFN_DIM ** -0.5).astype(jnp.bfloat16)
    x_norm = jax.random.normal(part_keys[0], (TOKENS, HIDDEN), jnp.float32).astype(jnp.bfloat16)
    u_gate = jax.random.normal(part_keys[1], (TOKENS, FFN_DIM), jnp.float32).astype(jnp.bfloat16)
    u_up = jax.random.normal(part_keys[2], (TOKENS, FFN_DIM), jnp.float32).astype(jnp.bfloat16)
    grad_out = jax.random.normal(part_keys[3], (TOKENS, HIDDEN), jnp.float32).astype(jnp.bfloat16)
    return dict(x_norm=x_norm, w_gate=w_gate, w_up=w_up, w_down=w_down, u_gate=u_gate, u_up=u_up, grad_out=grad_out)


def reference(x_norm, w_gate, w_up, w_down, u_gate, u_up, grad_out):
    col_block = FFN_DIM // GROUP_SIZE
    wg_blocks = w_gate.reshape(HIDDEN, GROUP_SIZE, col_block).transpose(1, 0, 2)
    wu_blocks = w_up.reshape(HIDDEN, GROUP_SIZE, col_block).transpose(1, 0, 2)
    wd_blocks = w_down.reshape(GROUP_SIZE, col_block, HIDDEN)
    ug_blocks = u_gate.reshape(TOKENS, GROUP_SIZE, col_block).transpose(1, 0, 2)
    uu_blocks = u_up.reshape(TOKENS, GROUP_SIZE, col_block).transpose(1, 0, 2)

    def one_block(dx_acc, operands):
        wg_blk, wu_blk, wd_blk, ug_blk, uu_blk = operands
        gate_f = ug_blk.astype(jnp.float32)
        up_f = uu_blk.astype(jnp.float32)
        sigmoid_g = jax.nn.sigmoid(gate_f)
        silu_g = gate_f * sigmoid_g
        z_act = (silu_g * up_f).astype(jnp.bfloat16)
        grad_wd = jnp.dot(z_act.T, grad_out, preferred_element_type=jnp.float32)
        grad_mid = jnp.dot(grad_out, wd_blk.T, preferred_element_type=jnp.float32)
        d_gate = (grad_mid * up_f * sigmoid_g * (1.0 + gate_f * (1.0 - sigmoid_g))).astype(jnp.bfloat16)
        d_up = (grad_mid * silu_g).astype(jnp.bfloat16)
        partial = (jnp.dot(d_gate, wg_blk.T, preferred_element_type=jnp.float32)
                   + jnp.dot(d_up, wu_blk.T, preferred_element_type=jnp.float32)).astype(jnp.bfloat16)
        grad_wg = jnp.dot(x_norm.T, d_gate, preferred_element_type=jnp.float32)
        grad_wu = jnp.dot(x_norm.T, d_up, preferred_element_type=jnp.float32)
        return dx_acc + partial.astype(jnp.float32), (grad_wg, grad_wu, grad_wd)

    dx_init = jnp.zeros((TOKENS, HIDDEN), jnp.float32)
    dx_sum, stacked = lax.scan(one_block, dx_init, (wg_blocks, wu_blocks, wd_blocks, ug_blocks, uu_blocks))
    gw_gate, gw_up, gw_down = stacked
    grad_x = dx_sum.astype(jnp.bfloat16)
    grad_w_gate = gw_gate.transpose(1, 0, 2).reshape(HIDDEN, FFN_DIM)
    grad_w_up = gw_up.transpose(1, 0, 2).reshape(HIDDEN, FFN_DIM)
    grad_w_down = gw_down.reshape(FFN_DIM, HIDDEN)
    return (grad_x, grad_w_gate, grad_w_up, grad_w_down)
```

```python
import jax
import jax.numpy as jnp
from jax import lax
from jax.experimental import pallas as pl
from jax.experimental.pallas import tpu as pltpu
from jax.sharding import PartitionSpec as P

F32 = jnp.float32
BF16 = jnp.bfloat16
CHUNKS = 2
NT = (((1,), (1,)), ((), ()))
NN = (((1,), (0,)), ((), ()))
VMEM_LIMIT = 60 * 1024 * 1024


def _call(body, *, flops, nbytes, deps=(), in_specs=None, **kw):
    if in_specs is not None:
        n = len(in_specs)
        kw['in_specs'] = list(in_specs) + [pl.BlockSpec(memory_space=pl.ANY)] * len(deps)
        inner = body

        def body(*refs):
            inner(*refs[:n], *refs[n + len(deps):])

    call = pl.pallas_call(
        body,
        compiler_params=pltpu.CompilerParams(vmem_limit_bytes=VMEM_LIMIT),
        cost_estimate=pl.CostEstimate(flops=flops, bytes_accessed=nbytes, transcendentals=0),
        **kw)
    return lambda *args: call(*args, *deps)


def _resident(shape):
    return pl.BlockSpec(shape, lambda i: (0,) * len(shape), pipeline_mode=pl.Buffered(1))


def _z_body(ug_ref, uu_ref, zt_ref):
    gate = ug_ref[0].astype(F32)
    z = (gate * jax.nn.sigmoid(gate) * uu_ref[0].astype(F32)).astype(BF16)
    zt_ref[...] = z.T


def _z_transposed(ug3, uu3, chunk, rows):
    group, tok, width = ug3.shape
    spec = pl.BlockSpec((1, rows, width), lambda i: (i, chunk, 0))
    return _call(
        _z_body, flops=group * rows * width * 8, nbytes=group * rows * width * 6,
        grid=(group,), in_specs=[spec, spec],
        out_specs=pl.BlockSpec((width, rows), lambda i: (0, i)),
        out_shape=jax.ShapeDtypeStruct((width, group * rows), BF16))(ug3, uu3)


def _mid_body(dy_ref, wd_ref, ug_ref, uu_ref, dg_ref, du_ref):
    pair, rows, hidden = dy_ref.shape
    width = wd_ref.shape[0]
    dy = dy_ref[...].reshape(pair * rows, hidden)
    step = 256
    for lo in range(0, width, step):
        cols = slice(lo, lo + step)
        g = lax.dot_general(dy, wd_ref[cols, :], NT, preferred_element_type=F32)
        gate = ug_ref[:, :, cols].reshape(pair * rows, step).astype(F32)
        up = uu_ref[:, :, cols].reshape(pair * rows, step).astype(F32)
        sig = jax.nn.sigmoid(gate)
        d_gate = (g * up * sig * (1.0 + gate * (1.0 - sig))).astype(BF16)
        d_up = (g * (gate * sig)).astype(BF16)
        dg_ref[:, :, cols] = d_gate.reshape(pair, rows, step)
        du_ref[:, :, cols] = d_up.reshape(pair, rows, step)


def _mid_grads(dy3, wd, ug3, uu3, chunk, deps):
    group, rows, hidden = dy3.shape
    width = wd.shape[0]
    u_spec = pl.BlockSpec((2, rows, width), lambda i: (i, chunk, 0))
    o_spec = pl.BlockSpec((2, rows, width), lambda i: (i, 0, 0))
    out = jax.ShapeDtypeStruct((group, rows, width), BF16)
    return _call(
        _mid_body, flops=2 * group * rows * hidden * width,
        nbytes=2 * (group * rows * (hidden + 4 * width) + width * hidden),
        deps=deps, grid=(group // 2,),
        in_specs=[pl.BlockSpec((2, rows, hidden), lambda i: (i, 0, 0)), _resident(wd.shape), u_spec, u_spec],
        out_specs=[o_spec, o_spec], out_shape=[out, out])(dy3, wd, ug3, uu3)


STEPS = ((1, 0), (1, 1), (0, 0), (0, 1))


def _partial_body(me_ref, dg_ref, du_ref, wg_ref, wu_ref, *rest):
    a_refs, b_refs, (buf, sems) = rest[:4], rest[4:8], rest[8:]
    _, rows, width = dg_ref.shape
    hidden = wg_ref.shape[0]
    half = hidden // 2
    i = pl.program_id(0)
    slot = i % 2
    core = me_ref[2]

    def copies(k, at):
        rx, ry = STEPS[k]
        out = []
        for rc in range(2):
            out.append(pltpu.make_async_copy(
                buf.at[at, rc, :, :half], a_refs[rx * 2 + rc].at[ry], sems.at[at, 2 * rc]))
            out.append(pltpu.make_async_copy(
                buf.at[at, rc, :, half:], b_refs[ry * 2 + rc].at[rx], sems.at[at, 2 * rc + 1]))
        return out

    for k in range(2, 4):
        @pl.when(i == k)
        def _():
            for c in copies(k - 2, k % 2):
                c.wait()

    dg = jnp.concatenate([dg_ref[core], dg_ref[1 - core]], axis=0)
    du = jnp.concatenate([du_ref[core], du_ref[1 - core]], axis=0)
    step = 512
    for lo in range(0, hidden, step):
        cols = slice(lo, lo + step)
        acc = (lax.dot_general(dg, wg_ref[cols, :], NT, preferred_element_type=F32)
               + lax.dot_general(du, wu_ref[cols, :], NT, preferred_element_type=F32))
        buf[slot, :, :, cols] = acc.astype(BF16).reshape(2, rows, step)

    for k in range(4):
        @pl.when(i == k)
        def _():
            for c in copies(k, k % 2):
                c.start()

    @pl.when(i == 3)
    def _():
        for k in (2, 3):
            for c in copies(k, k % 2):
                c.wait()


def _partials(me, dg3, du3, wg, wu):
    group, rows, width = dg3.shape
    hidden = wg.shape[0]
    half = hidden // 2

    def chip(i, me_ref):
        rx, ry = 1 - i // 2, i % 2
        return ((me_ref[0] + ry) % 2 * 2 + (me_ref[1] + rx) % 2, 0, 0)

    d_spec = pl.BlockSpec((2, rows, width), chip)
    w_spec = pl.BlockSpec(wg.shape, lambda i, me_ref: (0, 0), pipeline_mode=pl.Buffered(1))
    out = jax.ShapeDtypeStruct((2, rows, half), BF16)
    outs = _call(
        _partial_body, flops=4 * group * rows * hidden * width,
        nbytes=2 * (group * rows * (hidden + 2 * width) + 2 * width * hidden),
        grid_spec=pltpu.PrefetchScalarGridSpec(
            num_scalar_prefetch=1, grid=(4,),
            in_specs=[d_spec, d_spec, w_spec, w_spec],
            out_specs=[pl.BlockSpec(memory_space=pl.ANY)] * 8,
            scratch_shapes=[pltpu.VMEM((2, 2, rows, hidden), BF16), pltpu.SemaphoreType.DMA((2, 4))]),
        out_shape=[out] * 8)(me, dg3, du3, wg, wu)
    return outs[:4], outs[4:]


def _wdown_body(*refs):
    n = (len(refs) - 1) // 2
    o_ref = refs[-1]
    acc = None
    for zt_ref, dy_ref in zip(refs[:n], refs[n:2 * n]):
        part = lax.dot_general(zt_ref[...], dy_ref[...], NN, preferred_element_type=F32)
        acc = part if acc is None else acc + part
    o_ref[...] = acc


def _wdown(zts, dys, deps, step=512):
    width, tok = zts[0].shape
    hidden = dys[0].shape[1]
    n = len(zts)
    return _call(
        _wdown_body, flops=2 * n * tok * width * hidden,
        nbytes=n * 2 * tok * (width + hidden) + 4 * width * hidden,
        deps=deps, grid=(hidden // step,),
        in_specs=[_resident(zts[0].shape)] * n + [pl.BlockSpec((tok, step), lambda i: (0, i))] * n,
        out_specs=pl.BlockSpec((width, step), lambda i: (0, i)),
        out_shape=jax.ShapeDtypeStruct((width, hidden), F32))(*zts, *dys)


def _wcol_body(*refs):
    n = (len(refs) - 1) // 2
    o_ref = refs[-1]
    acc = None
    for x_ref, d_ref in zip(refs[:n], refs[n:2 * n]):
        group, _, rows, step = x_ref.shape
        xt = x_ref[...].reshape(group * rows, step).T
        part = lax.dot_general(xt, d_ref[...], NN, preferred_element_type=F32)
        acc = part if acc is None else acc + part
    o_ref[...] = acc


def _wcol(x4, ds, deps, step=512):
    group, n, rows, hidden = x4.shape
    tok, width = ds[0].shape

    def x_spec(h):
        return pl.BlockSpec((group, 1, rows, step), lambda i: (0, h, 0, i))

    return _call(
        _wcol_body, flops=2 * n * tok * width * hidden,
        nbytes=n * 2 * tok * (width + hidden) + 4 * width * hidden,
        deps=deps, grid=(hidden // step,),
        in_specs=[x_spec(h) for h in range(n)] + [_resident(ds[0].shape)] * n,
        out_specs=pl.BlockSpec((step, width), lambda i: (i, 0)),
        out_shape=jax.ShapeDtypeStruct((hidden, width), F32))(*([x4] * n), *ds)


def _sum4(refs):
    return refs[0][0].astype(F32) + refs[1][0].astype(F32) + refs[2][0].astype(F32) + refs[3][0].astype(F32)


def _away_body(*refs):
    refs[8][...] = _sum4(refs[:4])
    refs[9][...] = _sum4(refs[4:8])


def _away_sums(got_a, got_b, deps, step=512):
    _, rows, half = got_a[0].shape
    out = jax.ShapeDtypeStruct((rows, half), F32)
    o_spec = pl.BlockSpec((rows, step), lambda i: (0, i))
    return _call(
        _away_body, flops=8 * rows * half, nbytes=24 * rows * half, deps=deps, grid=(half // step,),
        in_specs=[pl.BlockSpec((1, rows, step), lambda i: (1, 0, i))] * 8,
        out_specs=[o_spec] * 2, out_shape=[out] * 2)(*got_a, *got_b)


def _final_body(*refs):
    half = refs[8].shape[1]
    refs[-1][:, :half] = (_sum4(refs[:4]) + refs[8][...]).astype(BF16)
    refs[-1][:, half:] = (_sum4(refs[4:8]) + refs[9][...]).astype(BF16)


def _final_sums(got_a, got_b, far_a, far_b, chunk, whole, deps, step=64):
    _, rows, half = got_a[0].shape
    aliased = [] if whole is None else [whole]
    n = 10 + len(aliased)
    return _call(
        _final_body, flops=8 * rows * half, nbytes=28 * rows * half, deps=deps, grid=(rows // step,),
        in_specs=[pl.BlockSpec((1, step, half), lambda i: (0, i, 0))] * 8
        + [pl.BlockSpec((step, half), lambda i: (i, 0))] * 2 + [pl.BlockSpec(memory_space=pl.ANY)] * len(aliased),
        out_specs=pl.BlockSpec((step, 2 * half), lambda i: (i + chunk * (rows // step), 0)),
        out_shape=jax.ShapeDtypeStruct((CHUNKS * rows, 2 * half), BF16),
        input_output_aliases={n - 1: 0} if aliased else {})(*got_a, *got_b, far_a, far_b, *aliased)


def solution(mesh):
    group = mesh.shape['tp']

    def send(value, away):
        return lax.ppermute(value, 'tp', [(d, d ^ away) for d in range(group)])

    def local_backward(x_loc, wg_loc, wu_loc, wd_loc, ug_loc, uu_loc, dy_loc):
        tok, hidden = x_loc.shape
        width = wd_loc.shape[0]
        rows = tok // CHUNKS
        me = lax.axis_index('tp')
        place = jnp.stack([me // 4, (me // 2) % 2, me % 2]).astype(jnp.int32)
        ug3 = ug_loc.reshape(group, tok, width)
        uu3 = uu_loc.reshape(group, tok, width)

        dys = [lax.all_gather(dy_loc[h * rows:(h + 1) * rows], 'tp', axis=0, tiled=True) for h in range(CHUNKS)]
        x_full = lax.all_gather(x_loc, 'tp', axis=0, tiled=True)
        zts = [_z_transposed(ug3, uu3, h, rows) for h in range(CHUNKS)]

        def first_stage(parts, near):
            return [parts[0]] + [send(parts[r], (r // 2) * near + r % 2) for r in range(1, 4)]

        dgs, dus, recvs, last = [], [], [], tuple(zts)
        for h in range(CHUNKS):
            dg3, du3 = _mid_grads(dys[h].reshape(group, rows, hidden), wd_loc, ug3, uu3, h, last)
            pa, pb = _partials(place, dg3, du3, wg_loc, wu_loc)
            last = (pa[0],)
            recvs.append((first_stage(pa, 2), first_stage(pb, 4)))
            dgs.append(dg3.reshape(group * rows, width))
            dus.append(du3.reshape(group * rows, width))

        def second_stage(h, deps):
            away_a, away_b = _away_sums(*recvs[h], deps)
            return (away_a,), (send(away_a, 4), send(away_b, 2))

        x4 = x_full.reshape(group, CHUNKS, rows, hidden)
        grad_wd = _wdown(zts, dys, last)
        last, far0 = second_stage(0, (grad_wd,))
        grad_wg = _wcol(x4, dgs, last)
        last, far1 = second_stage(1, (grad_wg,))
        grad_wu = _wcol(x4, dus, last)
        grad_x = _final_sums(*recvs[0], *far0, 0, None, (grad_wu,))
        grad_x = _final_sums(*recvs[1], *far1, 1, grad_x, ())
        return grad_x, grad_wg, grad_wu, grad_wd

    row_spec = P(('dp', 'tp'), None)
    col_spec = P(None, 'tp')
    part_cols = P('dp', 'tp')
    return jax.shard_map(local_backward, mesh=mesh,
                         in_specs=(row_spec, col_spec, col_spec, P('tp', None), part_cols, part_cols, row_spec),
                         out_specs=(row_spec, part_cols, part_cols, row_spec),
                         check_vma=False)
```

```python
import jax
import jax.numpy as jnp
from jax import lax
from jax.experimental import pallas as pl
from jax.experimental.pallas import tpu as pltpu
from jax.sharding import PartitionSpec as P

F32 = jnp.float32
BF16 = jnp.bfloat16
CHUNKS = 2
NT = (((1,), (1,)), ((), ()))
NN = (((1,), (0,)), ((), ()))
VMEM_LIMIT = 60 * 1024 * 1024


def _call(body, args, *, flops, nbytes, grid, in_specs, out_specs, out_shape, place=None, deps=(), aliases=None):
    n_in, n_dep, first = len(in_specs), len(deps), 0 if place is None else 1

    def kernel(*refs):
        body(*refs[first:first + n_in], *refs[first + n_in + n_dep:])

    return pl.pallas_call(
        kernel,
        grid_spec=pltpu.PrefetchScalarGridSpec(
            num_scalar_prefetch=first, grid=grid,
            in_specs=list(in_specs) + [pl.BlockSpec(memory_space=pl.ANY)] * n_dep, out_specs=out_specs),
        out_shape=out_shape,
        input_output_aliases=aliases or {},
        compiler_params=pltpu.CompilerParams(vmem_limit_bytes=VMEM_LIMIT),
        cost_estimate=pl.CostEstimate(flops=flops, bytes_accessed=nbytes, transcendentals=0),
    )(*([] if place is None else [place]), *args, *deps)


def _fixed(shape, *index):
    def at(i, *place):
        return tuple(place[0][int(e[1:])] if isinstance(e, str) else e for e in index)

    return pl.BlockSpec(shape, at, pipeline_mode=pl.Buffered(1))


def _along(shape, axis, *index, offset=0):
    def at(i, *place):
        out = [place[0][int(e[1:])] if isinstance(e, str) else e for e in index]
        out[axis] = i + offset
        return tuple(out)

    return pl.BlockSpec(shape, at)


def _value(ref):
    return ref[...].reshape(ref.shape[-2:]) if len(ref.shape) < 4 or ref.shape[1] == 1 else ref[...].reshape(-1, ref.shape[-1])


def _rows_of(refs):
    vals = [_value(r) for r in refs]
    return vals[0] if len(vals) == 1 else jnp.concatenate(vals, axis=0)


def _z_body(ug_ref, uu_ref, zt_ref):
    gate = ug_ref[0, 0].astype(F32)
    z = (gate * jax.nn.sigmoid(gate) * uu_ref[0, 0].astype(F32)).astype(BF16)
    zt_ref[...] = z.T


def _z_transposed(place, ug4, uu4, chunk, relative, deps):
    group, _, rows, width = ug4.shape
    spec = pl.BlockSpec((1, 1, rows, width), lambda i, p: (p[i] if relative else i, chunk, 0, 0))
    return _call(
        _z_body, (ug4, uu4), flops=group * rows * width * 8, nbytes=group * rows * width * 6, place=place, deps=deps,
        grid=(group,), in_specs=[spec, spec], out_specs=pl.BlockSpec((width, rows), lambda i, p: (0, i)),
        out_shape=jax.ShapeDtypeStruct((width, group * rows), BF16))


def _mid_grads(place, units, wd, ug4, uu4, deps, step=256):
    width, hidden = wd.shape
    rows = ug4.shape[2]
    n = len(units)
    pieces = [p for ps, _, _ in units for p in ps]
    counts = [len(ps) for ps, _, _ in units]

    def body(*refs):
        dy_refs, refs = refs[:len(pieces)], refs[len(pieces):]
        wd_ref, ug_refs, uu_refs, (dg_ref, du_ref) = refs[0], refs[1:1 + n], refs[1 + n:1 + 2 * n], refs[1 + 2 * n:]
        at = 0
        for u in range(0, n, 2):
            take = counts[u] + counts[u + 1]
            dy = _rows_of(dy_refs[at:at + take])
            at += take
            g2 = lax.dot_general(dy, wd_ref[...], NT, preferred_element_type=F32)
            for k in range(2):
                g = g2[k * rows:(k + 1) * rows]
                gate = ug_refs[u + k][0, 0].astype(F32)
                up = uu_refs[u + k][0, 0].astype(F32)
                sig = jax.nn.sigmoid(gate)
                dg_ref[u + k] = (g * up * sig * (1.0 + gate * (1.0 - sig))).astype(BF16)
                du_ref[u + k] = (g * (gate * sig)).astype(BF16)

    u_specs = [_along((1, 1, rows, step), 3, f'r{r}', h, 0, 0) for _, r, h in units]
    o_spec = _along((n, rows, step), 2, 0, 0, 0)
    out = jax.ShapeDtypeStruct((n, rows, width), BF16)
    return _call(
        body, [a for a, _ in pieces] + [wd] + [ug4] * n + [uu4] * n, place=place, deps=deps,
        flops=2 * n * rows * hidden * width, nbytes=2 * (n * rows * (hidden + 4 * width) + width * hidden),
        grid=(width // step,),
        in_specs=[s for _, s in pieces] + [_along((step, hidden), 0, 0, 0)] + u_specs + u_specs,
        out_specs=[o_spec, o_spec], out_shape=[out, out])


def _partials(dg3, du3, wg, wu, targets, shapes, deps=(), step=256):
    n, rows, width = dg3.shape
    hidden = wg.shape[0]
    half = hidden // 2

    def body(dg_ref, du_ref, wga_ref, wgb_ref, wua_ref, wub_ref, *outs):
        dg = dg_ref[...].reshape(n * rows, width)
        du = du_ref[...].reshape(n * rows, width)
        wg_t = jnp.concatenate([wga_ref[...], wgb_ref[...]], axis=0)
        wu_t = jnp.concatenate([wua_ref[...], wub_ref[...]], axis=0)
        acc = (lax.dot_general(dg, wg_t, NT, preferred_element_type=F32)
               + lax.dot_general(du, wu_t, NT, preferred_element_type=F32)).astype(BF16)
        for u, pair in enumerate(targets):
            for side, (o, lead) in enumerate(pair):
                outs[o][lead] = acc[u * rows:(u + 1) * rows, side * step:(side + 1) * step]

    tiles = half // step
    left, right = _along((step, width), 0, 0, 0), _along((step, width), 0, 0, 0, offset=tiles)
    return _call(
        body, (dg3, du3, wg, wg, wu, wu), deps=deps,
        flops=4 * n * rows * hidden * width, nbytes=2 * (n * rows * (hidden + 2 * width) + 2 * width * hidden),
        grid=(tiles,),
        in_specs=[_fixed(dg3.shape, 0, 0, 0), _fixed(du3.shape, 0, 0, 0), left, right, left, right],
        out_specs=[_along((m, rows, step), 2, 0, 0, 0) for m in shapes],
        out_shape=[jax.ShapeDtypeStruct((m, rows, half), BF16) for m in shapes])


def _wdown(zts, groups, deps, step=512):
    width, tok = zts[0].shape
    n = len(zts)
    counts = [len(g) for g in groups]
    pieces = [p for g in groups for p in g]
    hidden = pieces[0][0].shape[-1]

    def body(*refs):
        o_ref, acc, at = refs[-1], None, n
        for h in range(n):
            part = lax.dot_general(refs[h][...], _rows_of(refs[at:at + counts[h]]), NN, preferred_element_type=F32)
            at += counts[h]
            acc = part if acc is None else acc + part
        o_ref[...] = acc

    return _call(
        body, list(zts) + [a for a, _ in pieces], deps=deps,
        flops=2 * n * tok * width * hidden, nbytes=n * 2 * tok * (width + hidden) + 4 * width * hidden,
        grid=(hidden // step,),
        in_specs=[_fixed(z.shape, 0, 0) for z in zts] + [s for _, s in pieces],
        out_specs=_along((width, step), 1, 0, 0),
        out_shape=jax.ShapeDtypeStruct((width, hidden), F32))


def _wcol(place, x4, groups, deps, step=512):
    _, both, rows, hidden = x4.shape
    width = groups[0][0].shape[-1]
    n = len(groups)
    counts = [len(w) for _, w in groups]

    def body(*refs):
        o_ref, acc, at = refs[-1], None, n
        for g in range(n):
            xt = _rows_of(refs[at:at + counts[g]]).T
            at += counts[g]
            part = lax.dot_general(xt, refs[g][...], NN, preferred_element_type=F32)
            acc = part if acc is None else acc + part
        o_ref[...] = acc

    x_specs = []
    for _, where in groups:
        for r, h in where:
            x_specs.append(_along((1, both if h is None else 1, rows, step), 3, f'r{r}', h or 0, 0, 0))
    tok = sum(d.shape[0] for d, _ in groups)
    return _call(
        body, [d for d, _ in groups] + [x4] * len(x_specs), place=place, deps=deps,
        flops=2 * tok * width * hidden, nbytes=2 * tok * (width + hidden) + 4 * width * hidden,
        grid=(hidden // step,),
        in_specs=[_fixed(d.shape, 0, 0) for d, _ in groups] + x_specs,
        out_specs=_along((step, width), 0, 0, 0),
        out_shape=jax.ShapeDtypeStruct((hidden, width), F32))


def _sum(refs):
    total = refs[0][0].astype(F32)
    for r in refs[1:]:
        total = total + r[0].astype(F32)
    return total


def _away_sums(terms_a, terms_b, deps, step=512):
    _, rows, half = terms_a[0][0].shape
    n = len(terms_a)

    def body(*refs):
        refs[2 * n][...] = _sum(refs[:n])
        refs[2 * n + 1][...] = _sum(refs[n:2 * n])

    out = jax.ShapeDtypeStruct((rows, half), F32)
    o_spec = _along((rows, step), 1, 0, 0)
    return _call(
        body, [a for a, _ in terms_a + terms_b], flops=8 * rows * half, nbytes=24 * rows * half, deps=deps,
        grid=(half // step,), in_specs=[_along((1, rows, step), 2, k, 0, 0) for _, k in terms_a + terms_b],
        out_specs=[o_spec] * 2, out_shape=[out] * 2)


def _final_sums(terms_a, terms_b, far_a, far_b, chunk, whole, deps, step=64):
    rows, half = far_a.shape
    n = len(terms_a)
    steps = rows // step
    old = [] if whole is None else [whole]

    def body(*refs):
        o_ref = refs[-1]
        o_ref[:, :half] = (_sum(refs[:n]) + refs[2 * n][...]).astype(BF16)
        o_ref[:, half:] = (_sum(refs[n:2 * n]) + refs[2 * n + 1][...]).astype(BF16)

    args = [a for a, _ in terms_a + terms_b] + [far_a, far_b] + old
    return _call(
        body, args, flops=8 * rows * half, nbytes=28 * rows * half, deps=deps, grid=(steps,),
        in_specs=[_along((1, step, half), 1, k, 0, 0) for _, k in terms_a + terms_b]
        + [_along((step, half), 0, 0, 0)] * 2 + [pl.BlockSpec(memory_space=pl.ANY)] * len(old),
        out_specs=_along((step, 2 * half), 0, 0, 0, offset=chunk * steps),
        out_shape=jax.ShapeDtypeStruct((CHUNKS * rows, 2 * half), BF16),
        aliases={len(args) - 1: 0} if old else None)


def solution(mesh):
    group = mesh.shape['tp']

    def send(value, away):
        return lax.ppermute(value, 'tp', [(d, d ^ away) for d in range(group)])

    def local_backward(x_loc, wg_loc, wu_loc, wd_loc, ug_loc, uu_loc, dy_loc):
        tok, hidden = x_loc.shape
        width = wd_loc.shape[0]
        rows = tok // CHUNKS
        quarter = rows // 2
        place = lax.axis_index('tp').astype(jnp.int32) ^ jnp.arange(group, dtype=jnp.int32)
        ug4 = ug_loc.reshape(group, CHUNKS, rows, width)
        uu4 = uu_loc.reshape(group, CHUNKS, rows, width)

        dy0 = lax.all_gather(dy_loc[:rows], 'tp', axis=0, tiled=True)
        dy_mate = send(dy_loc, 1)
        dy_x0 = send(dy_loc[rows:], 2)
        dy_y0 = send(dy_loc[rows:], 4)
        x4 = lax.all_gather(x_loc, 'tp', axis=0, tiled=True).reshape(group, CHUNKS, rows, hidden)

        zt0 = _z_transposed(place, ug4, uu4, 0, False, ())

        def own(h):
            return _fixed((rows, hidden), h, 0)

        dg_own, du_own = _mid_grads(
            place, [([(a, own(h))], r, h) for r, a in ((0, dy_loc), (1, dy_mate)) for h in range(CHUNKS)],
            wd_loc, ug4, uu4, (zt0,))
        keep_a, keep_b, give_a, give_b = _partials(
            dg_own, du_own, wg_loc, wu_loc,
            [((0, 0), (1, 0)), ((0, 1), (1, 1)), ((2, 0), (3, 0)), ((2, 1), (3, 1))], [2, 2, 2, 2])
        mate_a, mate_b = send(give_a, 1), send(give_b, 1)
        zt1 = _z_transposed(place, ug4, uu4, 1, True, (keep_a,))

        dy_x0, dy_y0, zt1 = lax.optimization_barrier((dy_x0, dy_y0, zt1))

        via_x, via_y = dy_x0[:quarter], dy_y0[quarter:]
        dy_x1, dy_y1 = send(dy_x0, 1), send(dy_y0, 1)
        dy_d0 = [send(via_x, 4), send(via_y, 2)]

        def whole(a):
            return (a, _fixed(a.shape, 0, 0))

        dy03 = dy0.reshape(group, rows, hidden)
        units0 = [([(dy03, _fixed((1, rows, hidden), f'r{r}', 0, 0))], r, 0) for r in range(2, group)]
        targets = [((2, 0), (4, 0)), ((3, 0), (5, 0)), ((0, 0), (6, 0)), ((1, 0), (7, 0)),
                   ((2, 1), (6, 1)), ((3, 1), (7, 1))]
        dgs, dus, near, last = [], [], [], (zt1, via_x, via_y)
        for h in range(CHUNKS):
            dg3, du3 = _mid_grads(place, units1 if h else units0, wd_loc, ug4, uu4, last)
            if h == 0:
                dy_d0 = lax.optimization_barrier((*dy_d0, dg3))[:2]
                dy_d1 = [send(p, 1) for p in dy_d0]
                sources = [dy_x0], [dy_x1], [dy_y0], [dy_y1], dy_d0, dy_d1
                units1 = [([whole(a) for a in ps], r, 1) for r, ps in zip(range(2, group), sources)]
            p = _partials(dg3, du3, wg_loc, wu_loc, targets, [1, 1, 2, 2, 1, 1, 2, 2])
            last = (p[0],)
            near.append(((p[0], send(p[2], 2), send(p[3], 3), send(p[1], 1)),
                         (p[4], send(p[6], 4), send(p[7], 5), send(p[5], 1))))
            dgs.append(dg3.reshape(-1, width))
            dus.append(du3.reshape(-1, width))

        def far_sums(h, deps):
            a, b = ([(t[0], 0), (t[3], 0), (t[1], 1), (t[2], 1)] for t in near[h])
            away_a, away_b = _away_sums(a, b, deps)
            return (away_a,), (send(away_a, 4), send(away_b, 2))

        def finish(h, far, whole_dx, deps):
            a, b = ([(k, h), (m, h), (t[1], 0), (t[2], 0)]
                    for k, m, t in ((keep_a, mate_a, near[h][0]), (keep_b, mate_b, near[h][1])))
            return _final_sums(a, b, *far, h, whole_dx, deps)

        def cols(a, shape, *at):
            return (a, _along(shape, len(at) - 1, *at))

        strip = 512
        dy1 = [cols(a, (rows, strip), 1, 0) for a in (dy_loc, dy_mate)]
        dy1 += [cols(a, (a.shape[0], strip), 0, 0) for a in (dy_x0, dy_x1, dy_y0, dy_y1, *dy_d0, *dy_d1)]
        grad_wd = _wdown([zt0, zt1], [[cols(dy0, (group * rows, strip), 0, 0)], dy1], last, strip)

        def grad_col(own_rows, rest, deps):
            groups = [(own_rows.reshape(-1, width), [(0, None), (1, None)])]
            groups += [(rest[h], [(r, h) for r in range(2, group)]) for h in range(CHUNKS)]
            return _wcol(place, x4, groups, deps)

        grad_wg = grad_col(dg_own, dgs, (grad_wd,))
        last, far0 = far_sums(0, (grad_wg,))
        grad_wu = grad_col(du_own, dus, last)
        last, far1 = far_sums(1, (grad_wu,))
        grad_x = finish(0, far0, None, last)
        grad_x = finish(1, far1, grad_x, ())
        return grad_x, grad_wg, grad_wu, grad_wd

    row_spec = P(('dp', 'tp'), None)
    col_spec = P(None, 'tp')
    part_cols = P('dp', 'tp')
    return jax.shard_map(local_backward, mesh=mesh,
                         in_specs=(row_spec, col_spec, col_spec, P('tp', None), part_cols, part_cols, row_spec),
                         out_specs=(row_spec, part_cols, part_cols, row_spec),
                         check_vma=False)
```

```python
import jax
import jax.numpy as jnp
from jax import lax
from jax.experimental import pallas as pl
from jax.experimental.pallas import tpu as pltpu
from jax.sharding import PartitionSpec as P

F32 = jnp.float32
BF16 = jnp.bfloat16
CHUNKS = 2
NT = (((1,), (1,)), ((), ()))
NN = (((1,), (0,)), ((), ()))
VMEM_LIMIT = 60 * 1024 * 1024


def _call(body, args, *, flops, nbytes, grid, in_specs, out_specs, out_shape, place=None, deps=(), aliases=None):
    n_in, n_dep, first = len(in_specs), len(deps), 0 if place is None else 1

    def kernel(*refs):
        body(*refs[first:first + n_in], *refs[first + n_in + n_dep:])

    return pl.pallas_call(
        kernel,
        grid_spec=pltpu.PrefetchScalarGridSpec(
            num_scalar_prefetch=first, grid=grid,
            in_specs=list(in_specs) + [pl.BlockSpec(memory_space=pl.ANY)] * n_dep, out_specs=out_specs),
        out_shape=out_shape,
        input_output_aliases=aliases or {},
        compiler_params=pltpu.CompilerParams(vmem_limit_bytes=VMEM_LIMIT),
        cost_estimate=pl.CostEstimate(flops=flops, bytes_accessed=nbytes, transcendentals=0),
    )(*([] if place is None else [place]), *args, *deps)


def _fixed(shape, *index):
    def at(i, *place):
        return tuple(place[0][int(e[1:])] if isinstance(e, str) else e for e in index)

    return pl.BlockSpec(shape, at, pipeline_mode=pl.Buffered(1))


def _along(shape, axis, *index, offset=0):
    def at(i, *place):
        out = [place[0][int(e[1:])] if isinstance(e, str) else e for e in index]
        out[axis] = i + offset
        return tuple(out)

    return pl.BlockSpec(shape, at)


def _value(ref):
    return ref[...].reshape(ref.shape[-2:]) if len(ref.shape) < 4 or ref.shape[1] == 1 else ref[...].reshape(-1, ref.shape[-1])


def _rows_of(refs):
    vals = [_value(r) for r in refs]
    return vals[0] if len(vals) == 1 else jnp.concatenate(vals, axis=0)


def _z_body(ug_ref, uu_ref, *rest):
    _, both, rows, width = ug_ref.shape
    gate = ug_ref[...].reshape(both * rows, width).astype(F32)
    z = gate * jax.nn.sigmoid(gate) * uu_ref[...].reshape(both * rows, width).astype(F32)
    rest[-1][...] = z.astype(BF16).T


def _z_transposed(place, ug4, uu4, first, count, old, deps):
    group, both, rows, width = ug4.shape
    tok = both * rows
    spec = pl.BlockSpec((1, both, rows, width), lambda i, p: (p[i + first], 0, 0, 0))
    args = [ug4, uu4] + ([] if old is None else [old])
    return _call(
        _z_body, args, flops=count * tok * width * 8, nbytes=count * tok * width * 6, place=place, deps=deps,
        grid=(count,), in_specs=[spec, spec] + [pl.BlockSpec(memory_space=pl.ANY)] * (len(args) - 2),
        out_specs=pl.BlockSpec((width, tok), lambda i, p: (0, i + first)),
        out_shape=jax.ShapeDtypeStruct((width, group * tok), BF16),
        aliases=None if old is None else {3: 0})


def _mid_grads(place, units, wd, ug4, uu4, lead, old, deps, step=256):
    width, hidden = wd.shape
    rows = ug4.shape[2]
    n = len(units)
    pieces = [p for ps, _, _ in units for p in ps]
    counts = [len(ps) for ps, _, _ in units]

    def body(*refs):
        dy_refs, refs = refs[:len(pieces)], refs[len(pieces):]
        wd_ref, ug_refs, uu_refs, (dg_ref, du_ref) = refs[0], refs[1:1 + n], refs[1 + n:1 + 2 * n], refs[-2:]
        at = 0
        for u in range(0, n, 2):
            take = counts[u] + counts[u + 1]
            dy = _rows_of(dy_refs[at:at + take])
            at += take
            g2 = lax.dot_general(dy, wd_ref[...], NT, preferred_element_type=F32)
            for k in range(2):
                g = g2[k * rows:(k + 1) * rows]
                gate = ug_refs[u + k][0, 0].astype(F32)
                up = uu_refs[u + k][0, 0].astype(F32)
                sig = jax.nn.sigmoid(gate)
                dg_ref[u + k] = (g * up * sig * (1.0 + gate * (1.0 - sig))).astype(BF16)
                du_ref[u + k] = (g * (gate * sig)).astype(BF16)

    u_specs = [_along((1, 1, rows, step), 3, f'r{r}', h, 0, 0) for _, r, h in units]
    o_spec = _along((n, rows, step), 2, lead, 0, 0)
    out = jax.ShapeDtypeStruct((ug4.shape[0] * ug4.shape[1], rows, width), BF16)
    args = [a for a, _ in pieces] + [wd] + [ug4] * n + [uu4] * n + list(old)
    return _call(
        body, args, place=place, deps=deps, aliases={len(args) - 1: 0, len(args): 1} if old else None,
        flops=2 * n * rows * hidden * width, nbytes=2 * (n * rows * (hidden + 4 * width) + width * hidden),
        grid=(width // step,),
        in_specs=[s for _, s in pieces] + [_along((step, hidden), 0, 0, 0)] + u_specs + u_specs
        + [pl.BlockSpec(memory_space=pl.ANY)] * len(old),
        out_specs=[o_spec, o_spec], out_shape=[out, out])


def _partials(dg3, du3, lead, wg, wu, targets, shapes, deps=(), step=256):
    n, (_, rows, width) = len(targets), dg3.shape
    hidden = wg.shape[0]
    half = hidden // 2

    def body(dg_ref, du_ref, wga_ref, wgb_ref, wua_ref, wub_ref, *outs):
        dg = dg_ref[...].reshape(n * rows, width)
        du = du_ref[...].reshape(n * rows, width)
        wg_t = jnp.concatenate([wga_ref[...], wgb_ref[...]], axis=0)
        wu_t = jnp.concatenate([wua_ref[...], wub_ref[...]], axis=0)
        acc = (lax.dot_general(dg, wg_t, NT, preferred_element_type=F32)
               + lax.dot_general(du, wu_t, NT, preferred_element_type=F32)).astype(BF16)
        for u, pair in enumerate(targets):
            for side, (o, lead) in enumerate(pair):
                outs[o][lead] = acc[u * rows:(u + 1) * rows, side * step:(side + 1) * step]

    tiles = half // step
    left, right = _along((step, width), 0, 0, 0), _along((step, width), 0, 0, 0, offset=tiles)
    return _call(
        body, (dg3, du3, wg, wg, wu, wu), deps=deps,
        flops=4 * n * rows * hidden * width, nbytes=2 * (n * rows * (hidden + 2 * width) + 2 * width * hidden),
        grid=(tiles,),
        in_specs=[_fixed((n, rows, width), lead, 0, 0)] * 2 + [left, right, left, right],
        out_specs=[_along((m, rows, step), 2, 0, 0, 0) for m in shapes],
        out_shape=[jax.ShapeDtypeStruct((m, rows, half), BF16) for m in shapes])


def _wdown(zt, pieces, deps, step=512):
    width, tok = zt.shape
    hidden = pieces[0][0].shape[-1]

    def body(zt_ref, *refs):
        refs[-1][...] = lax.dot_general(zt_ref[...], _rows_of(refs[:-1]), NN, preferred_element_type=F32)

    return _call(
        body, [zt] + [a for a, _ in pieces], deps=deps,
        flops=2 * tok * width * hidden, nbytes=2 * tok * (width + hidden) + 4 * width * hidden,
        grid=(hidden // step,), in_specs=[_fixed(zt.shape, 0, 0)] + [s for _, s in pieces],
        out_specs=_along((width, step), 1, 0, 0),
        out_shape=jax.ShapeDtypeStruct((width, hidden), F32))


def _wcol(place, x4, d_rows, order, deps, step=512):
    _, both, rows, hidden = x4.shape
    tok, width = d_rows.shape

    def body(d_ref, *refs):
        xt = _rows_of(refs[:-1]).T
        refs[-1][...] = lax.dot_general(xt, d_ref[...], NN, preferred_element_type=F32)

    return _call(
        body, [d_rows] + [x4] * len(order), place=place, deps=deps,
        flops=2 * tok * width * hidden, nbytes=2 * tok * (width + hidden) + 4 * width * hidden,
        grid=(hidden // step,),
        in_specs=[_fixed(d_rows.shape, 0, 0)] + [_along((1, both, rows, step), 3, f'r{r}', 0, 0, 0) for r in order],
        out_specs=_along((step, width), 0, 0, 0),
        out_shape=jax.ShapeDtypeStruct((hidden, width), F32))


def _sum(refs):
    total = refs[0][0].astype(F32)
    for r in refs[1:]:
        total = total + r[0].astype(F32)
    return total


def _away_sums(terms_a, terms_b, deps, step=512):
    _, rows, half = terms_a[0][0].shape
    n = len(terms_a)

    def body(*refs):
        refs[2 * n][...] = _sum(refs[:n])
        refs[2 * n + 1][...] = _sum(refs[n:2 * n])

    out = jax.ShapeDtypeStruct((rows, half), F32)
    o_spec = _along((rows, step), 1, 0, 0)
    return _call(
        body, [a for a, _ in terms_a + terms_b], flops=8 * rows * half, nbytes=24 * rows * half, deps=deps,
        grid=(half // step,), in_specs=[_along((1, rows, step), 2, k, 0, 0) for _, k in terms_a + terms_b],
        out_specs=[o_spec] * 2, out_shape=[out] * 2)


def _final_sums(terms_a, terms_b, far_a, far_b, chunk, whole, deps, step=64):
    rows, half = far_a.shape
    n = len(terms_a)
    steps = rows // step
    old = [] if whole is None else [whole]

    def body(*refs):
        o_ref = refs[-1]
        o_ref[:, :half] = (_sum(refs[:n]) + refs[2 * n][...]).astype(BF16)
        o_ref[:, half:] = (_sum(refs[n:2 * n]) + refs[2 * n + 1][...]).astype(BF16)

    args = [a for a, _ in terms_a + terms_b] + [far_a, far_b] + old
    return _call(
        body, args, flops=8 * rows * half, nbytes=28 * rows * half, deps=deps, grid=(steps,),
        in_specs=[_along((1, step, half), 1, k, 0, 0) for _, k in terms_a + terms_b]
        + [_along((step, half), 0, 0, 0)] * 2 + [pl.BlockSpec(memory_space=pl.ANY)] * len(old),
        out_specs=_along((step, 2 * half), 0, 0, 0, offset=chunk * steps),
        out_shape=jax.ShapeDtypeStruct((CHUNKS * rows, 2 * half), BF16),
        aliases={len(args) - 1: 0} if old else None)


def solution(mesh):
    group = mesh.shape['tp']

    def send(value, away):
        return lax.ppermute(value, 'tp', [(d, d ^ away) for d in range(group)])

    def local_backward(x_loc, wg_loc, wu_loc, wd_loc, ug_loc, uu_loc, dy_loc):
        tok, hidden = x_loc.shape
        width = wd_loc.shape[0]
        rows = tok // CHUNKS
        place = lax.axis_index('tp').astype(jnp.int32) ^ jnp.arange(group, dtype=jnp.int32)
        ug4 = ug_loc.reshape(group, CHUNKS, rows, width)
        uu4 = uu_loc.reshape(group, CHUNKS, rows, width)
        hs = range(CHUNKS)

        dy_mate, dy_x0, dy_y0 = send(dy_loc, 1), send(dy_loc, 2), send(dy_loc, 4)
        zt = _z_transposed(place, ug4, uu4, 0, 4, None, ())

        def piece(a, h=0):
            return ([(a, _fixed((rows, hidden), h, 0))],)

        units = [piece(a, h) + (r, h) for r, a in ((0, dy_loc), (1, dy_mate)) for h in hs]
        dg, du = _mid_grads(place, units, wd_loc, ug4, uu4, 2, (), (zt,))
        keep_a, keep_b, give_a, give_b = _partials(
            dg, du, 2, wg_loc, wu_loc,
            [((0, 0), (1, 0)), ((0, 1), (1, 1)), ((2, 0), (3, 0)), ((2, 1), (3, 1))], [2, 2, 2, 2])
        mate_a, mate_b = send(give_a, 1), send(give_b, 1)
        dy_x0, dy_y0, keep_a, x_later = lax.optimization_barrier((dy_x0, dy_y0, keep_a, x_loc))
        x4 = lax.all_gather(x_later, 'tp', axis=0, tiled=True).reshape(group, CHUNKS, rows, hidden)

        dy_x1, dy_y1 = send(dy_x0, 1), send(dy_y0, 1)
        via_x, via_y = dy_x0[:rows], dy_y0[rows:]
        dy_d0 = [send(via_x, 4), send(via_y, 2)]
        zt = _z_transposed(place, ug4, uu4, 4, 4, zt, (keep_a, via_x, via_y))

        near = ((2, dy_x0), (3, dy_x1), (4, dy_y0), (5, dy_y1))
        units = [piece(a, h) + (r, h) for r, a in near for h in hs]
        dg, du = _mid_grads(place, units, wd_loc, ug4, uu4, 0, (dg, du), (zt, keep_a))
        dy_d0 = lax.optimization_barrier((*dy_d0, dg))[:2]
        dy_d1 = [send(p, 1) for p in dy_d0]
        sides = ((0, 2), (1, 3), (6, 4), (7, 5))
        p = _partials(dg, du, 0, wg_loc, wu_loc, [((a, h), (b, h)) for a, b in sides for h in hs], [2] * 8)
        done_a = [keep_a, mate_a, send(p[0], 2), send(p[1], 3)]
        done_b = [keep_b, mate_b, send(p[4], 4), send(p[5], 5)]
        pass_a, pass_b = [p[6], send(p[7], 1)], [p[2], send(p[3], 1)]

        units = [piece(a) + (r, h) for r, ps in ((6, dy_d0), (7, dy_d1)) for h, a in enumerate(ps)]
        dg, du = _mid_grads(place, units, wd_loc, ug4, uu4, 3, (dg, du), (p[0],))
        q = _partials(dg, du, 3, wg_loc, wu_loc,
                      [((4 * k + h, 0), (4 * k + 2 + h, 0)) for k in range(2) for h in hs], [1] * 8)
        diag_a = [(send(q[h], 2), send(q[4 + h], 3)) for h in hs]
        diag_b = [(send(q[2 + h], 4), send(q[6 + h], 5)) for h in hs]

        def far_sums(h, deps):
            a, b = ([(w[0], h), (w[1], h), (d[h][0], 0), (d[h][1], 0)] for w, d in ((pass_a, diag_a), (pass_b, diag_b)))
            away_a, away_b = _away_sums(a, b, deps)
            return (away_a,), (send(away_a, 4), send(away_b, 2))

        def finish(h, far, whole_dx, deps):
            return _final_sums([(t, h) for t in done_a], [(t, h) for t in done_b], *far, h, whole_dx, deps)

        strip = 512

        def cols(a):
            return (a, _along((a.shape[0], strip), 1, 0, 0))

        grad_wd = _wdown(zt, [cols(a) for a in (dy_loc, dy_mate, dy_x0, dy_x1, dy_y0, dy_y1, *dy_d0, *dy_d1)],
                         (q[0],), strip)
        order = (2, 3, 4, 5, 0, 1, 6, 7)
        grad_wg = _wcol(place, x4, dg.reshape(-1, width), order, (grad_wd,))
        last, far0 = far_sums(0, (grad_wg,))
        last, far1 = far_sums(1, last)
        grad_wu = _wcol(place, x4, du.reshape(-1, width), order, last)
        grad_x = finish(0, far0, None, (grad_wu,))
        grad_x = finish(1, far1, grad_x, ())
        return grad_x, grad_wg, grad_wu, grad_wd

    row_spec = P(('dp', 'tp'), None)
    col_spec = P(None, 'tp')
    part_cols = P('dp', 'tp')
    return jax.shard_map(local_backward, mesh=mesh,
                         in_specs=(row_spec, col_spec, col_spec, P('tp', None), part_cols, part_cols, row_spec),
                         out_specs=(row_spec, part_cols, part_cols, row_spec),
                         check_vma=False)
```

```python
import jax
import jax.numpy as jnp
from jax import lax
from jax.experimental import pallas as pl
from jax.experimental.pallas import tpu as pltpu
from jax.sharding import PartitionSpec as P

F32 = jnp.float32
BF16 = jnp.bfloat16
CHUNKS = 2
NT = (((1,), (1,)), ((), ()))
NN = (((1,), (0,)), ((), ()))
VMEM_LIMIT = 60 * 1024 * 1024


def _call(body, args, *, flops, nbytes, grid, in_specs, out_specs, out_shape, place=None, deps=(), aliases=None):
    n_in, n_dep, first = len(in_specs), len(deps), 0 if place is None else 1

    def kernel(*refs):
        body(*refs[first:first + n_in], *refs[first + n_in + n_dep:])

    return pl.pallas_call(
        kernel,
        grid_spec=pltpu.PrefetchScalarGridSpec(
            num_scalar_prefetch=first, grid=grid,
            in_specs=list(in_specs) + [pl.BlockSpec(memory_space=pl.ANY)] * n_dep, out_specs=out_specs),
        out_shape=out_shape,
        input_output_aliases=aliases or {},
        compiler_params=pltpu.CompilerParams(vmem_limit_bytes=VMEM_LIMIT),
        cost_estimate=pl.CostEstimate(flops=flops, bytes_accessed=nbytes, transcendentals=0),
    )(*([] if place is None else [place]), *args, *deps)


def _fixed(shape, *index):
    def at(i, *place):
        return tuple(place[0][int(e[1:])] if isinstance(e, str) else e for e in index)

    return pl.BlockSpec(shape, at, pipeline_mode=pl.Buffered(1))


def _along(shape, axis, *index, offset=0):
    def at(i, *place):
        out = [place[0][int(e[1:])] if isinstance(e, str) else e for e in index]
        out[axis] = i + offset
        return tuple(out)

    return pl.BlockSpec(shape, at)


def _value(ref):
    return ref[...].reshape(ref.shape[-2:]) if len(ref.shape) < 4 or ref.shape[1] == 1 else ref[...].reshape(-1, ref.shape[-1])


def _rows_of(refs):
    vals = [_value(r) for r in refs]
    return vals[0] if len(vals) == 1 else jnp.concatenate(vals, axis=0)


def _z_body(ug_ref, uu_ref, *rest):
    _, both, rows, width = ug_ref.shape
    gate = ug_ref[...].reshape(both * rows, width).astype(F32)
    z = gate * jax.nn.sigmoid(gate) * uu_ref[...].reshape(both * rows, width).astype(F32)
    rest[-1][...] = z.astype(BF16).T


def _z_transposed(place, ug4, uu4, first, count, old, deps):
    group, both, rows, width = ug4.shape
    tok = both * rows
    spec = pl.BlockSpec((1, both, rows, width), lambda i, p: (p[i + first], 0, 0, 0))
    args = [ug4, uu4] + ([] if old is None else [old])
    return _call(
        _z_body, args, flops=count * tok * width * 8, nbytes=count * tok * width * 6, place=place, deps=deps,
        grid=(count,), in_specs=[spec, spec] + [pl.BlockSpec(memory_space=pl.ANY)] * (len(args) - 2),
        out_specs=pl.BlockSpec((width, tok), lambda i, p: (0, i + first)),
        out_shape=jax.ShapeDtypeStruct((width, group * tok), BF16),
        aliases=None if old is None else {3: 0})


def _mid_grads(place, units, wd, ug4, uu4, lead, old, deps, step=256):
    width, hidden = wd.shape
    rows = ug4.shape[2]
    n = len(units)
    pieces = [p for ps, _, _ in units for p in ps]
    counts = [len(ps) for ps, _, _ in units]

    def body(*refs):
        dy_refs, refs = refs[:len(pieces)], refs[len(pieces):]
        wd_ref, ug_refs, uu_refs, (dg_ref, du_ref) = refs[0], refs[1:1 + n], refs[1 + n:1 + 2 * n], refs[-2:]
        at = 0
        for u in range(0, n, 2):
            take = counts[u] + counts[u + 1]
            dy = _rows_of(dy_refs[at:at + take])
            at += take
            g2 = lax.dot_general(dy, wd_ref[...], NT, preferred_element_type=F32)
            for k in range(2):
                g = g2[k * rows:(k + 1) * rows]
                gate = ug_refs[u + k][0, 0].astype(F32)
                up = uu_refs[u + k][0, 0].astype(F32)
                sig = jax.nn.sigmoid(gate)
                dg_ref[u + k] = (g * up * sig * (1.0 + gate * (1.0 - sig))).astype(BF16)
                du_ref[u + k] = (g * (gate * sig)).astype(BF16)

    u_specs = [_along((1, 1, rows, step), 3, f'r{r}', h, 0, 0) for _, r, h in units]
    o_spec = _along((n, rows, step), 2, lead, 0, 0)
    out = jax.ShapeDtypeStruct((ug4.shape[0] * ug4.shape[1], rows, width), BF16)
    args = [a for a, _ in pieces] + [wd] + [ug4] * n + [uu4] * n + list(old)
    return _call(
        body, args, place=place, deps=deps, aliases={len(args) - 1: 0, len(args): 1} if old else None,
        flops=2 * n * rows * hidden * width, nbytes=2 * (n * rows * (hidden + 4 * width) + width * hidden),
        grid=(width // step,),
        in_specs=[s for _, s in pieces] + [_along((step, hidden), 0, 0, 0)] + u_specs + u_specs
        + [pl.BlockSpec(memory_space=pl.ANY)] * len(old),
        out_specs=[o_spec, o_spec], out_shape=[out, out])


def _partials(dg3, du3, lead, wg, wu, targets, shapes, deps=(), step=256):
    n, (_, rows, width) = len(targets), dg3.shape
    hidden = wg.shape[0]
    half = hidden // 2

    def body(dg_ref, du_ref, wga_ref, wgb_ref, wua_ref, wub_ref, *outs):
        dg = dg_ref[...].reshape(n * rows, width)
        du = du_ref[...].reshape(n * rows, width)
        wg_t = jnp.concatenate([wga_ref[...], wgb_ref[...]], axis=0)
        wu_t = jnp.concatenate([wua_ref[...], wub_ref[...]], axis=0)
        acc = (lax.dot_general(dg, wg_t, NT, preferred_element_type=F32)
               + lax.dot_general(du, wu_t, NT, preferred_element_type=F32)).astype(BF16)
        for u, pair in enumerate(targets):
            for side, (o, lead) in enumerate(pair):
                outs[o][lead] = acc[u * rows:(u + 1) * rows, side * step:(side + 1) * step]

    tiles = half // step
    left, right = _along((step, width), 0, 0, 0), _along((step, width), 0, 0, 0, offset=tiles)
    return _call(
        body, (dg3, du3, wg, wg, wu, wu), deps=deps,
        flops=4 * n * rows * hidden * width, nbytes=2 * (n * rows * (hidden + 2 * width) + 2 * width * hidden),
        grid=(tiles,),
        in_specs=[_fixed((n, rows, width), lead, 0, 0)] * 2 + [left, right, left, right],
        out_specs=[_along((m, rows, step), 2, 0, 0, 0) for m in shapes],
        out_shape=[jax.ShapeDtypeStruct((m, rows, half), BF16) for m in shapes])


def _wdown(zt, pieces, deps, step=512):
    width, tok = zt.shape
    hidden = pieces[0][0].shape[-1]

    def body(zt_ref, *refs):
        refs[-1][...] = lax.dot_general(zt_ref[...], _rows_of(refs[:-1]), NN, preferred_element_type=F32)

    return _call(
        body, [zt] + [a for a, _ in pieces], deps=deps,
        flops=2 * tok * width * hidden, nbytes=2 * tok * (width + hidden) + 4 * width * hidden,
        grid=(hidden // step,), in_specs=[_fixed(zt.shape, 0, 0)] + [s for _, s in pieces],
        out_specs=_along((width, step), 1, 0, 0),
        out_shape=jax.ShapeDtypeStruct((width, hidden), F32))


def _wcol(place, x4, d_rows, order, deps, step=512):
    _, both, rows, hidden = x4.shape
    tok, width = d_rows.shape

    def body(d_ref, *refs):
        xt = _rows_of(refs[:-1]).T
        refs[-1][...] = lax.dot_general(xt, d_ref[...], NN, preferred_element_type=F32)

    return _call(
        body, [d_rows] + [x4] * len(order), place=place, deps=deps,
        flops=2 * tok * width * hidden, nbytes=2 * tok * (width + hidden) + 4 * width * hidden,
        grid=(hidden // step,),
        in_specs=[_fixed(d_rows.shape, 0, 0)] + [_along((1, both, rows, step), 3, f'r{r}', 0, 0, 0) for r in order],
        out_specs=_along((step, width), 0, 0, 0),
        out_shape=jax.ShapeDtypeStruct((hidden, width), F32))


def _sum(refs):
    total = refs[0][...].astype(F32)
    for r in refs[1:]:
        total = total + r[...].astype(F32)
    return total


def _far_sums(terms_a, terms_b, deps, step=512):
    both, rows, half = terms_a[0].shape
    n = len(terms_a)

    def body(*refs):
        refs[2 * n][...] = _sum(refs[:n])
        refs[2 * n + 1][...] = _sum(refs[n:2 * n])

    spec = _along((both, rows, step), 2, 0, 0, 0)
    return _call(
        body, [*terms_a, *terms_b], flops=16 * rows * half, nbytes=48 * rows * half, deps=deps,
        grid=(half // step,), in_specs=[spec] * (2 * n), out_specs=[spec] * 2,
        out_shape=[jax.ShapeDtypeStruct((both, rows, half), F32)] * 2)


def _final_sums(terms_a, terms_b, far_a, far_b, deps, step=64):
    both, rows, half = far_a.shape
    n = len(terms_a)
    steps = rows // step

    def body(*refs):
        refs[-1][:, :half] = (_sum(refs[:n]) + refs[2 * n][...]).astype(BF16).reshape(step, half)
        refs[-1][:, half:] = (_sum(refs[n:2 * n]) + refs[2 * n + 1][...]).astype(BF16).reshape(step, half)

    spec = pl.BlockSpec((1, step, half), lambda i: (i // steps, i % steps, 0))
    return _call(
        body, [*terms_a, *terms_b, far_a, far_b], flops=16 * rows * half, nbytes=56 * rows * half, deps=deps,
        grid=(both * steps,), in_specs=[spec] * (2 * n + 2), out_specs=_along((step, 2 * half), 0, 0, 0),
        out_shape=jax.ShapeDtypeStruct((both * rows, 2 * half), BF16))


def solution(mesh):
    group = mesh.shape['tp']

    def send(value, away):
        return lax.ppermute(value, 'tp', [(d, d ^ away) for d in range(group)])

    def local_backward(x_loc, wg_loc, wu_loc, wd_loc, ug_loc, uu_loc, dy_loc):
        tok, hidden = x_loc.shape
        width = wd_loc.shape[0]
        rows = tok // CHUNKS
        place = lax.axis_index('tp').astype(jnp.int32) ^ jnp.arange(group, dtype=jnp.int32)
        ug4 = ug_loc.reshape(group, CHUNKS, rows, width)
        uu4 = uu_loc.reshape(group, CHUNKS, rows, width)
        hs = range(CHUNKS)

        dy_mate, dy_x0, dy_y0 = send(dy_loc, 1), send(dy_loc, 2), send(dy_loc, 4)
        zt = _z_transposed(place, ug4, uu4, 0, 4, None, ())

        def piece(a, h=0):
            return ([(a, _fixed((rows, hidden), h, 0))],)

        units = [piece(a, h) + (r, h) for r, a in ((0, dy_loc), (1, dy_mate)) for h in hs]
        dg, du = _mid_grads(place, units, wd_loc, ug4, uu4, 2, (), (zt,))
        keep_a, keep_b, give_a, give_b = _partials(
            dg, du, 2, wg_loc, wu_loc,
            [((0, 0), (1, 0)), ((0, 1), (1, 1)), ((2, 0), (3, 0)), ((2, 1), (3, 1))], [2, 2, 2, 2])
        mate_a, mate_b = send(give_a, 1), send(give_b, 1)
        dy_x0, dy_y0, keep_a, x_later = lax.optimization_barrier((dy_x0, dy_y0, keep_a, x_loc))
        x4 = lax.all_gather(x_later, 'tp', axis=0, tiled=True).reshape(group, CHUNKS, rows, hidden)

        dy_x1, dy_y1 = send(dy_x0, 1), send(dy_y0, 1)
        via_x, via_y = dy_x0[:rows], dy_y0[rows:]
        dy_d0 = [send(via_x, 4), send(via_y, 2)]
        zt = _z_transposed(place, ug4, uu4, 4, 4, zt, (keep_a, via_x, via_y))

        near = ((2, dy_x0), (3, dy_x1), (4, dy_y0), (5, dy_y1))
        units = [piece(a, h) + (r, h) for r, a in near for h in hs]
        dg, du = _mid_grads(place, units, wd_loc, ug4, uu4, 0, (dg, du), (zt, keep_a))
        sides = ((0, 2), (1, 3), (6, 4), (7, 5))
        p = _partials(dg, du, 0, wg_loc, wu_loc, [((a, h), (b, h)) for a, b in sides for h in hs], [2] * 8)
        dy_d0 = lax.optimization_barrier((*dy_d0, p[0]))[:2]
        dy_d1 = [send(a, 1) for a in dy_d0]
        done_a = [keep_a, mate_a, send(p[0], 2), send(p[1], 3)]
        done_b = [keep_b, mate_b, send(p[4], 4), send(p[5], 5)]
        pass_a, pass_b = [p[6], send(p[7], 1)], [p[2], send(p[3], 1)]

        units = [piece(a) + (r, h) for r, ps in ((6, dy_d0), (7, dy_d1)) for h, a in enumerate(ps)]
        dg, du = _mid_grads(place, units, wd_loc, ug4, uu4, 3, (dg, du), (p[0],))
        q = _partials(dg, du, 3, wg_loc, wu_loc, [((2 * k, h), (2 * k + 1, h)) for k in range(2) for h in hs], [2] * 4)
        pass_a += [send(q[0], 2), send(q[2], 3)]
        pass_b += [send(q[1], 4), send(q[3], 5)]

        strip = 512

        def cols(a):
            return (a, _along((a.shape[0], strip), 1, 0, 0))

        grad_wd = _wdown(zt, [cols(a) for a in (dy_loc, dy_mate, dy_x0, dy_x1, dy_y0, dy_y1, *dy_d0, *dy_d1)],
                         (q[0],), strip)
        order = (2, 3, 4, 5, 0, 1, 6, 7)
        grad_wg = _wcol(place, x4, dg.reshape(-1, width), order, (grad_wd,))
        far_a, far_b = _far_sums(pass_a, pass_b, (grad_wg,))
        grad_wu = _wcol(place, x4, du.reshape(-1, width), order, (far_a,))
        grad_x = _final_sums(done_a, done_b, send(far_a, 4), send(far_b, 2), (grad_wu,))
        return grad_x, grad_wg, grad_wu, grad_wd

    row_spec = P(('dp', 'tp'), None)
    col_spec = P(None, 'tp')
    part_cols = P('dp', 'tp')
    return jax.shard_map(local_backward, mesh=mesh,
                         in_specs=(row_spec, col_spec, col_spec, P('tp', None), part_cols, part_cols, row_spec),
                         out_specs=(row_spec, part_cols, part_cols, row_spec),
                         check_vma=False)
```

```python
import jax
import jax.numpy as jnp
from jax import lax
from jax.experimental import pallas as pl
from jax.experimental.pallas import tpu as pltpu
from jax.sharding import PartitionSpec as P


F32 = jnp.float32
BF16 = jnp.bfloat16
CHUNKS = 2
NT = (((1,), (1,)), ((), ()))
NN = (((1,), (0,)), ((), ()))
VMEM_LIMIT = 60 * 1024 * 1024


def _call(body, args, *, flops, nbytes, grid, in_specs, out_specs, out_shape, place=None, deps=(), aliases=None):
    n_in, n_dep, first = len(in_specs), len(deps), 0 if place is None else 1

    def kernel(*refs):
        body(*refs[first:first + n_in], *refs[first + n_in + n_dep:])

    return pl.pallas_call(
        kernel,
        grid_spec=pltpu.PrefetchScalarGridSpec(
            num_scalar_prefetch=first, grid=grid,
            in_specs=list(in_specs) + [pl.BlockSpec(memory_space=pl.ANY)] * n_dep, out_specs=out_specs),
        out_shape=out_shape,
        input_output_aliases=aliases or {},
        compiler_params=pltpu.CompilerParams(vmem_limit_bytes=VMEM_LIMIT),
        cost_estimate=pl.CostEstimate(flops=flops, bytes_accessed=nbytes, transcendentals=0),
    )(*([] if place is None else [place]), *args, *deps)


def _fixed(shape, *index):
    def at(i, *place):
        return tuple(place[0][int(e[1:])] if isinstance(e, str) else e for e in index)

    return pl.BlockSpec(shape, at, pipeline_mode=pl.Buffered(1))


def _along(shape, axis, *index, offset=0):
    def at(i, *place):
        out = [place[0][int(e[1:])] if isinstance(e, str) else e for e in index]
        out[axis] = i + offset
        return tuple(out)

    return pl.BlockSpec(shape, at)


def _value(ref):
    return ref[...].reshape(ref.shape[-2:]) if len(ref.shape) < 4 or ref.shape[1] == 1 else ref[...].reshape(-1, ref.shape[-1])


def _rows_of(refs):
    vals = [_value(r) for r in refs]
    return vals[0] if len(vals) == 1 else jnp.concatenate(vals, axis=0)


def _z_body(ug_ref, uu_ref, *rest):
    _, both, rows, width = ug_ref.shape
    gate = ug_ref[...].reshape(both * rows, width).astype(F32)
    z = gate * jax.nn.sigmoid(gate) * uu_ref[...].reshape(both * rows, width).astype(F32)
    rest[-1][...] = z.astype(BF16).T


def _z_transposed(place, ug4, uu4, first, count, old, deps):
    group, both, rows, width = ug4.shape
    tok = both * rows
    spec = pl.BlockSpec((1, both, rows, width), lambda i, p: (p[i + first], 0, 0, 0))
    args = [ug4, uu4] + ([] if old is None else [old])
    return _call(
        _z_body, args, flops=count * tok * width * 8, nbytes=count * tok * width * 6, place=place, deps=deps,
        grid=(count,), in_specs=[spec, spec] + [pl.BlockSpec(memory_space=pl.ANY)] * (len(args) - 2),
        out_specs=pl.BlockSpec((width, tok), lambda i, p: (0, i + first)),
        out_shape=jax.ShapeDtypeStruct((width, group * tok), BF16),
        aliases=None if old is None else {3: 0})


def _mid_grads(place, units, wd, ug4, uu4, lead, old, deps, step=256):
    width, hidden = wd.shape
    rows = ug4.shape[2]
    n = len(units)
    pieces = [p for ps, _, _ in units for p in ps]
    counts = [len(ps) for ps, _, _ in units]

    def body(*refs):
        dy_refs, refs = refs[:len(pieces)], refs[len(pieces):]
        wd_ref, ug_refs, uu_refs, (dg_ref, du_ref) = refs[0], refs[1:1 + n], refs[1 + n:1 + 2 * n], refs[-2:]
        at = 0
        for u in range(0, n, 2):
            take = counts[u] + counts[u + 1]
            dy = _rows_of(dy_refs[at:at + take])
            at += take
            g2 = lax.dot_general(dy, wd_ref[...], NT, preferred_element_type=F32)
            for k in range(2):
                g = g2[k * rows:(k + 1) * rows]
                gate = ug_refs[u + k][0, 0].astype(F32)
                up = uu_refs[u + k][0, 0].astype(F32)
                sig = jax.nn.sigmoid(gate)
                dg_ref[u + k] = (g * up * sig * (1.0 + gate * (1.0 - sig))).astype(BF16)
                du_ref[u + k] = (g * (gate * sig)).astype(BF16)

    u_specs = [_along((1, 1, rows, step), 3, f'r{r}', h, 0, 0) for _, r, h in units]
    o_spec = _along((n, rows, step), 2, lead, 0, 0)
    out = jax.ShapeDtypeStruct((ug4.shape[0] * ug4.shape[1], rows, width), BF16)
    args = [a for a, _ in pieces] + [wd] + [ug4] * n + [uu4] * n + list(old)
    return _call(
        body, args, place=place, deps=deps, aliases={len(args) - 1: 0, len(args): 1} if old else None,
        flops=2 * n * rows * hidden * width, nbytes=2 * (n * rows * (hidden + 4 * width) + width * hidden),
        grid=(width // step,),
        in_specs=[s for _, s in pieces] + [_along((step, hidden), 0, 0, 0)] + u_specs + u_specs
        + [pl.BlockSpec(memory_space=pl.ANY)] * len(old),
        out_specs=[o_spec, o_spec], out_shape=[out, out])


def _partials(dg3, du3, lead, wg, wu, targets, shapes, deps=(), step=256):
    n, (_, rows, width) = len(targets), dg3.shape
    hidden = wg.shape[0]
    half = hidden // 2

    def body(dg_ref, du_ref, wga_ref, wgb_ref, wua_ref, wub_ref, *outs):
        dg = dg_ref[...].reshape(n * rows, width)
        du = du_ref[...].reshape(n * rows, width)
        wg_t = jnp.concatenate([wga_ref[...], wgb_ref[...]], axis=0)
        wu_t = jnp.concatenate([wua_ref[...], wub_ref[...]], axis=0)
        acc = (lax.dot_general(dg, wg_t, NT, preferred_element_type=F32)
               + lax.dot_general(du, wu_t, NT, preferred_element_type=F32)).astype(BF16)
        for u, pair in enumerate(targets):
            for side, (o, lead) in enumerate(pair):
                outs[o][lead] = acc[u * rows:(u + 1) * rows, side * step:(side + 1) * step]

    tiles = half // step
    left, right = _along((step, width), 0, 0, 0), _along((step, width), 0, 0, 0, offset=tiles)
    return _call(
        body, (dg3, du3, wg, wg, wu, wu), deps=deps,
        flops=4 * n * rows * hidden * width, nbytes=2 * (n * rows * (hidden + 2 * width) + 2 * width * hidden),
        grid=(tiles,),
        in_specs=[_fixed((n, rows, width), lead, 0, 0)] * 2 + [left, right, left, right],
        out_specs=[_along((m, rows, step), 2, 0, 0, 0) for m in shapes],
        out_shape=[jax.ShapeDtypeStruct((m, rows, half), BF16) for m in shapes])


def _wdown(zt, pieces, deps, step=512):
    width, tok = zt.shape
    hidden = pieces[0][0].shape[-1]

    def body(zt_ref, *refs):
        refs[-1][...] = lax.dot_general(zt_ref[...], _rows_of(refs[:-1]), NN, preferred_element_type=F32)

    return _call(
        body, [zt] + [a for a, _ in pieces], deps=deps,
        flops=2 * tok * width * hidden, nbytes=2 * tok * (width + hidden) + 4 * width * hidden,
        grid=(hidden // step,), in_specs=[_fixed(zt.shape, 0, 0)] + [s for _, s in pieces],
        out_specs=_along((width, step), 1, 0, 0),
        out_shape=jax.ShapeDtypeStruct((width, hidden), F32))


def _wcol(d_rows, pieces, deps, step=512):
    tok, width = d_rows.shape
    hidden = pieces[0][0].shape[-1]

    def body(d_ref, *refs):
        xt = _rows_of(refs[:-1]).T
        refs[-1][...] = lax.dot_general(xt, d_ref[...], NN, preferred_element_type=F32)

    return _call(
        body, [d_rows] + [a for a, _ in pieces], deps=deps,
        flops=2 * tok * width * hidden, nbytes=2 * tok * (width + hidden) + 4 * width * hidden,
        grid=(hidden // step,), in_specs=[_fixed(d_rows.shape, 0, 0)] + [s for _, s in pieces],
        out_specs=_along((step, width), 0, 0, 0),
        out_shape=jax.ShapeDtypeStruct((hidden, width), F32))


def _sum(refs):
    total = refs[0][...].astype(F32)
    for r in refs[1:]:
        total = total + r[...].astype(F32)
    return total


def _far_sums(terms_a, terms_b, deps, step=512):
    both, rows, half = terms_a[0].shape
    n = len(terms_a)

    def body(*refs):
        for side, terms in enumerate((refs[:n], refs[n:2 * n])):
            total = _sum(terms)
            for h in range(both):
                refs[2 * n + side * both + h][...] = total[h]

    spec = _along((both, rows, step), 2, 0, 0, 0)
    return _call(
        body, [*terms_a, *terms_b], flops=16 * rows * half, nbytes=48 * rows * half, deps=deps,
        grid=(half // step,), in_specs=[spec] * (2 * n), out_specs=[_along((rows, step), 1, 0, 0)] * (2 * both),
        out_shape=[jax.ShapeDtypeStruct((rows, half), F32)] * (2 * both))


def _final_sums(terms_a, terms_b, far_a, far_b, chunk, whole, deps, step=64):
    rows, half = far_a.shape
    n = len(terms_a)
    steps = rows // step
    old = [] if whole is None else [whole]

    def body(*refs):
        o_ref = refs[-1]
        o_ref[:, :half] = (_sum(refs[:n])[0] + refs[2 * n][...]).astype(BF16)
        o_ref[:, half:] = (_sum(refs[n:2 * n])[0] + refs[2 * n + 1][...]).astype(BF16)

    args = [*terms_a, *terms_b, far_a, far_b] + old
    return _call(
        body, args, flops=8 * rows * half, nbytes=28 * rows * half, deps=deps, grid=(steps,),
        in_specs=[_along((1, step, half), 1, chunk, 0, 0)] * (2 * n)
        + [_along((step, half), 0, 0, 0)] * 2 + [pl.BlockSpec(memory_space=pl.ANY)] * len(old),
        out_specs=_along((step, 2 * half), 0, 0, 0, offset=chunk * steps),
        out_shape=jax.ShapeDtypeStruct((CHUNKS * rows, 2 * half), BF16),
        aliases={len(args) - 1: 0} if old else None)


def solution(mesh):
    group = mesh.shape['tp']

    def send(value, away):
        return lax.ppermute(value, 'tp', [(d, d ^ away) for d in range(group)])


    def layer(x_loc, wg_loc, wu_loc, wd_loc, ug_loc, uu_loc, dy_loc):
        tok, hidden = x_loc.shape
        width = wd_loc.shape[0]
        rows = tok // CHUNKS
        place = lax.axis_index('tp').astype(jnp.int32) ^ jnp.arange(group, dtype=jnp.int32)
        ug4 = ug_loc.reshape(group, CHUNKS, rows, width)
        uu4 = uu_loc.reshape(group, CHUNKS, rows, width)
        hs = range(CHUNKS)

        dy_mate = send(dy_loc, 1)
        halves = [dy_loc[:rows], dy_loc[rows:]]
        dy_x, dy_y = [None, None], [None, None]
        for h in hs:
            dy_x[h] = send(halves[h], 2)
            dy_y[1 - h] = send(halves[1 - h], 4)
        zt = _z_transposed(place, ug4, uu4, 0, 4, None, ())

        def piece(a, h=0):
            return ([(a, _fixed((rows, hidden), h, 0))],)

        units = [piece(a, h) + (r, h) for r, a in ((0, dy_loc), (1, dy_mate)) for h in hs]
        dg, du = _mid_grads(place, units, wd_loc, ug4, uu4, 2, (), (zt,))
        dy_x[0], dy_y[1], dg = lax.optimization_barrier((dy_x[0], dy_y[1], dg))
        dy_d = [send(dy_x[0], 4), send(dy_y[1], 2)]
        keep_a, keep_b, give_a, give_b = _partials(
            dg, du, 2, wg_loc, wu_loc,
            [((0, 0), (1, 0)), ((0, 1), (1, 1)), ((2, 0), (3, 0)), ((2, 1), (3, 1))], [2, 2, 2, 2])
        mate_a, mate_b = send(give_a, 1), send(give_b, 1)
        x_now, keep_a = lax.optimization_barrier((x_loc, keep_a))
        x_x0, x_y0 = send(x_now, 2), send(x_now, 4)
        dy_x[1], dy_y[0], keep_a = lax.optimization_barrier((dy_x[1], dy_y[0], keep_a))
        dy_xm, dy_ym = [send(a, 1) for a in dy_x], [send(a, 1) for a in dy_y]
        zt = _z_transposed(place, ug4, uu4, 4, 4, zt, (keep_a, dy_x[1], dy_y[0]))

        near = ((2, dy_x), (3, dy_xm), (4, dy_y), (5, dy_ym))
        units = [piece(ps[h]) + (r, h) for r, ps in near for h in hs]
        dg, du = _mid_grads(place, units, wd_loc, ug4, uu4, 0, (dg, du), (zt, keep_a))
        dy_d = list(lax.optimization_barrier((*dy_d, dg))[:2])
        dy_dm = [send(a, 1) for a in dy_d]
        sides = ((0, 2), (1, 3), (6, 4), (7, 5))
        targets = [((a, h), (b, h)) for a, b in sides for h in hs]
        p = _partials(dg, du, 0, wg_loc, wu_loc, targets, [2] * 8)
        x_x0, x_y0, near_x, near_y, x_own = lax.optimization_barrier((x_x0, x_y0, p[0], p[4], x_loc))
        x_d = [send(x_x0[:rows], 4), send(x_y0[rows:], 2)]
        x_mate, x_x1, x_y1 = send(x_own, 1), send(x_x0, 1), send(x_y0, 1)
        near_x, near_y = send(near_x, 2), send(near_y, 4)
        pass_a, pass_b = [p[6], send(p[7], 1)], [p[2], send(p[3], 1)]

        units = [piece(a) + (r, h) for r, ps in ((6, dy_d), (7, dy_dm)) for h, a in enumerate(ps)]
        dg, du = _mid_grads(place, units, wd_loc, ug4, uu4, 3, (dg, du), (p[0],))
        targets = [((2 * k, h), (2 * k + 1, h)) for k in range(2) for h in hs]
        q = _partials(dg, du, 3, wg_loc, wu_loc, targets, [2] * 4)
        pass_a += [send(q[0], 2), send(q[2], 3)]
        pass_b += [send(q[1], 4), send(q[3], 5)]

        late_x, late_y, _ = lax.optimization_barrier((p[1], p[5], q[0]))
        done_a = [keep_a, mate_a, near_x, send(late_x, 3)]
        done_b = [keep_b, mate_b, near_y, send(late_y, 5)]

        x_d = list(lax.optimization_barrier((*x_d, q[0]))[:2])
        x_dm = [send(a, 1) for a in x_d]
        strip = 512

        def cols(a):
            return (a, _along((a.shape[0], strip), 1, 0, 0))

        dy_rows = [cols(a) for a in (dy_loc, dy_mate, *dy_x, *dy_xm, *dy_y, *dy_ym, *dy_d, *dy_dm)]
        grad_wd = _wdown(zt, dy_rows, (q[0],), strip)
        x_rows = [cols(a) for a in (x_x0, x_x1, x_y0, x_y1, x_loc, x_mate, *x_d, *x_dm)]
        grad_wg = _wcol(dg.reshape(-1, width), x_rows, (grad_wd,))
        far = _far_sums(pass_a, pass_b, (grad_wg,))
        far_a, far_b = [send(a, 4) for a in far[:2]], [send(a, 2) for a in far[2:]]
        grad_wu = _wcol(du.reshape(-1, width), x_rows, (far[0],))
        grad_x = _final_sums(done_a, done_b, far_a[0], far_b[0], 0, None, (grad_wu,))
        grad_x = _final_sums(done_a, done_b, far_a[1], far_b[1], 1, grad_x, ())
        return grad_x, grad_wg, grad_wu, grad_wd

    row_spec = P(('dp', 'tp'), None)
    col_spec = P(None, 'tp')
    part_cols = P('dp', 'tp')
    return jax.shard_map(layer, mesh=mesh,
                         in_specs=(row_spec, col_spec, col_spec, P('tp', None), part_cols, part_cols, row_spec),
                         out_specs=(row_spec, part_cols, part_cols, row_spec),
                         check_vma=False)
```

```python
import jax
import jax.numpy as jnp
from jax import lax
from jax.experimental import pallas as pl
from jax.experimental.pallas import tpu as pltpu
from jax.sharding import PartitionSpec as P


F32 = jnp.float32
BF16 = jnp.bfloat16
CHUNKS = 2
NT = (((1,), (1,)), ((), ()))
NN = (((1,), (0,)), ((), ()))
VMEM_LIMIT = 60 * 1024 * 1024


def _call(body, args, *, flops, nbytes, grid, in_specs, out_specs, out_shape, place=None, deps=(), aliases=None):
    n_in, n_dep, first = len(in_specs), len(deps), 0 if place is None else 1

    def kernel(*refs):
        body(*refs[first:first + n_in], *refs[first + n_in + n_dep:])

    return pl.pallas_call(
        kernel,
        grid_spec=pltpu.PrefetchScalarGridSpec(
            num_scalar_prefetch=first, grid=grid,
            in_specs=list(in_specs) + [pl.BlockSpec(memory_space=pl.ANY)] * n_dep, out_specs=out_specs),
        out_shape=out_shape,
        input_output_aliases=aliases or {},
        compiler_params=pltpu.CompilerParams(vmem_limit_bytes=VMEM_LIMIT),
        cost_estimate=pl.CostEstimate(flops=flops, bytes_accessed=nbytes, transcendentals=0),
    )(*([] if place is None else [place]), *args, *deps)


def _fixed(shape, *index):
    def at(i, *place):
        return tuple(place[0][int(e[1:])] if isinstance(e, str) else e for e in index)

    return pl.BlockSpec(shape, at, pipeline_mode=pl.Buffered(1))


def _along(shape, axis, *index, offset=0):
    def at(i, *place):
        out = [place[0][int(e[1:])] if isinstance(e, str) else e for e in index]
        out[axis] = i + offset
        return tuple(out)

    return pl.BlockSpec(shape, at)


def _value(ref):
    return ref[...].reshape(ref.shape[-2:]) if len(ref.shape) < 4 or ref.shape[1] == 1 else ref[...].reshape(-1, ref.shape[-1])


def _rows_of(refs):
    vals = [_value(r) for r in refs]
    return vals[0] if len(vals) == 1 else jnp.concatenate(vals, axis=0)


def _z_body(ug_ref, uu_ref, *rest):
    _, both, rows, width = ug_ref.shape
    gate = ug_ref[...].reshape(both * rows, width).astype(F32)
    z = gate * jax.nn.sigmoid(gate) * uu_ref[...].reshape(both * rows, width).astype(F32)
    rest[-1][...] = z.astype(BF16).T


def _z_transposed(place, ug4, uu4, first, count, old, deps):
    group, both, rows, width = ug4.shape
    tok = both * rows
    spec = pl.BlockSpec((1, both, rows, width), lambda i, p: (p[i + first], 0, 0, 0))
    args = [ug4, uu4] + ([] if old is None else [old])
    return _call(
        _z_body, args, flops=count * tok * width * 8, nbytes=count * tok * width * 6, place=place, deps=deps,
        grid=(count,), in_specs=[spec, spec] + [pl.BlockSpec(memory_space=pl.ANY)] * (len(args) - 2),
        out_specs=pl.BlockSpec((width, tok), lambda i, p: (0, i + first)),
        out_shape=jax.ShapeDtypeStruct((width, group * tok), BF16),
        aliases=None if old is None else {3: 0})


def _mid_grads(place, units, wd, ug4, uu4, lead, old, deps, step=256):
    width, hidden = wd.shape
    rows = ug4.shape[2]
    n = len(units)
    pieces = [p for ps, _, _ in units for p in ps]
    counts = [len(ps) for ps, _, _ in units]

    def body(*refs):
        dy_refs, refs = refs[:len(pieces)], refs[len(pieces):]
        wd_ref, ug_refs, uu_refs, (dg_ref, du_ref) = refs[0], refs[1:1 + n], refs[1 + n:1 + 2 * n], refs[-2:]
        at = 0
        for u in range(0, n, 2):
            take = counts[u] + counts[u + 1]
            dy = _rows_of(dy_refs[at:at + take])
            at += take
            g2 = lax.dot_general(dy, wd_ref[...], NT, preferred_element_type=F32)
            for k in range(2):
                g = g2[k * rows:(k + 1) * rows]
                gate = ug_refs[u + k][0, 0].astype(F32)
                up = uu_refs[u + k][0, 0].astype(F32)
                sig = jax.nn.sigmoid(gate)
                dg_ref[u + k] = (g * up * sig * (1.0 + gate * (1.0 - sig))).astype(BF16)
                du_ref[u + k] = (g * (gate * sig)).astype(BF16)

    u_specs = [_along((1, 1, rows, step), 3, f'r{r}', h, 0, 0) for _, r, h in units]
    o_spec = _along((n, rows, step), 2, lead, 0, 0)
    out = jax.ShapeDtypeStruct((ug4.shape[0] * ug4.shape[1], rows, width), BF16)
    args = [a for a, _ in pieces] + [wd] + [ug4] * n + [uu4] * n + list(old)
    return _call(
        body, args, place=place, deps=deps, aliases={len(args) - 1: 0, len(args): 1} if old else None,
        flops=2 * n * rows * hidden * width, nbytes=2 * (n * rows * (hidden + 4 * width) + width * hidden),
        grid=(width // step,),
        in_specs=[s for _, s in pieces] + [_along((step, hidden), 0, 0, 0)] + u_specs + u_specs
        + [pl.BlockSpec(memory_space=pl.ANY)] * len(old),
        out_specs=[o_spec, o_spec], out_shape=[out, out])


def _partials(dg3, du3, lead, wg, wu, targets, shapes, deps=(), step=256):
    n, (_, rows, width) = len(targets), dg3.shape
    hidden = wg.shape[0]
    half = hidden // 2

    def body(dg_ref, du_ref, wga_ref, wgb_ref, wua_ref, wub_ref, *outs):
        dg = dg_ref[...].reshape(n * rows, width)
        du = du_ref[...].reshape(n * rows, width)
        wg_t = jnp.concatenate([wga_ref[...], wgb_ref[...]], axis=0)
        wu_t = jnp.concatenate([wua_ref[...], wub_ref[...]], axis=0)
        acc = (lax.dot_general(dg, wg_t, NT, preferred_element_type=F32)
               + lax.dot_general(du, wu_t, NT, preferred_element_type=F32)).astype(BF16)
        for u, pair in enumerate(targets):
            for side, (o, lead) in enumerate(pair):
                outs[o][lead] = acc[u * rows:(u + 1) * rows, side * step:(side + 1) * step]

    tiles = half // step
    left, right = _along((step, width), 0, 0, 0), _along((step, width), 0, 0, 0, offset=tiles)
    return _call(
        body, (dg3, du3, wg, wg, wu, wu), deps=deps,
        flops=4 * n * rows * hidden * width, nbytes=2 * (n * rows * (hidden + 2 * width) + 2 * width * hidden),
        grid=(tiles,),
        in_specs=[_fixed((n, rows, width), lead, 0, 0)] * 2 + [left, right, left, right],
        out_specs=[_along((m, rows, step), 2, 0, 0, 0) for m in shapes],
        out_shape=[jax.ShapeDtypeStruct((m, rows, half), BF16) for m in shapes])


def _wdown(zt, pieces, deps, step=512):
    width, tok = zt.shape
    hidden = pieces[0][0].shape[-1]

    def body(zt_ref, *refs):
        refs[-1][...] = lax.dot_general(zt_ref[...], _rows_of(refs[:-1]), NN, preferred_element_type=F32)

    return _call(
        body, [zt] + [a for a, _ in pieces], deps=deps,
        flops=2 * tok * width * hidden, nbytes=2 * tok * (width + hidden) + 4 * width * hidden,
        grid=(hidden // step,), in_specs=[_fixed(zt.shape, 0, 0)] + [s for _, s in pieces],
        out_specs=_along((width, step), 1, 0, 0),
        out_shape=jax.ShapeDtypeStruct((width, hidden), F32))


def _wcol(d_rows, pieces, deps, step=512):
    tok, width = d_rows.shape
    hidden = pieces[0][0].shape[-1]

    def body(d_ref, *refs):
        xt = _rows_of(refs[:-1]).T
        refs[-1][...] = lax.dot_general(xt, d_ref[...], NN, preferred_element_type=F32)

    return _call(
        body, [d_rows] + [a for a, _ in pieces], deps=deps,
        flops=2 * tok * width * hidden, nbytes=2 * tok * (width + hidden) + 4 * width * hidden,
        grid=(hidden // step,), in_specs=[_fixed(d_rows.shape, 0, 0)] + [s for _, s in pieces],
        out_specs=_along((step, width), 0, 0, 0),
        out_shape=jax.ShapeDtypeStruct((hidden, width), F32))


def _sum(refs):
    total = refs[0][...].astype(F32)
    for r in refs[1:]:
        total = total + r[...].astype(F32)
    return total


def _far_sums(terms_a, terms_b, chunk, deps, step=512):
    _, rows, half = terms_a[0].shape
    n = len(terms_a)

    def body(*refs):
        refs[2 * n][...] = _sum(refs[:n])[0]
        refs[2 * n + 1][...] = _sum(refs[n:2 * n])[0]

    return _call(
        body, [*terms_a, *terms_b], flops=8 * rows * half, nbytes=24 * rows * half, deps=deps,
        grid=(half // step,), in_specs=[_along((1, rows, step), 2, chunk, 0, 0)] * (2 * n),
        out_specs=[_along((rows, step), 1, 0, 0)] * 2, out_shape=[jax.ShapeDtypeStruct((rows, half), F32)] * 2)


def _final_sums(terms_a, terms_b, far_a, far_b, chunk, whole, deps, step=64):
    rows, half = far_a.shape
    n = len(terms_a)
    steps = rows // step
    old = [] if whole is None else [whole]

    def body(*refs):
        o_ref = refs[-1]
        o_ref[:, :half] = (_sum(refs[:n])[0] + refs[2 * n][...]).astype(BF16)
        o_ref[:, half:] = (_sum(refs[n:2 * n])[0] + refs[2 * n + 1][...]).astype(BF16)

    args = [*terms_a, *terms_b, far_a, far_b] + old
    return _call(
        body, args, flops=8 * rows * half, nbytes=28 * rows * half, deps=deps, grid=(steps,),
        in_specs=[_along((1, step, half), 1, chunk, 0, 0)] * (2 * n)
        + [_along((step, half), 0, 0, 0)] * 2 + [pl.BlockSpec(memory_space=pl.ANY)] * len(old),
        out_specs=_along((step, 2 * half), 0, 0, 0, offset=chunk * steps),
        out_shape=jax.ShapeDtypeStruct((CHUNKS * rows, 2 * half), BF16),
        aliases={len(args) - 1: 0} if old else None)


def solution(mesh):
    group = mesh.shape['tp']

    def send(value, away):
        return lax.ppermute(value, 'tp', [(d, d ^ away) for d in range(group)])


    def layer(x_loc, wg_loc, wu_loc, wd_loc, ug_loc, uu_loc, dy_loc):
        tok, hidden = x_loc.shape
        width = wd_loc.shape[0]
        rows = tok // CHUNKS
        place = lax.axis_index('tp').astype(jnp.int32) ^ jnp.arange(group, dtype=jnp.int32)
        ug4 = ug_loc.reshape(group, CHUNKS, rows, width)
        uu4 = uu_loc.reshape(group, CHUNKS, rows, width)
        hs = range(CHUNKS)

        dy_mate = send(dy_loc, 1)
        halves = [dy_loc[:rows], dy_loc[rows:]]
        dy_x, dy_y = [None, None], [None, None]
        for h in hs:
            dy_x[h] = send(halves[h], 2)
            dy_y[1 - h] = send(halves[1 - h], 4)
        zt = _z_transposed(place, ug4, uu4, 0, 4, None, ())

        def piece(a, h=0):
            return ([(a, _fixed((rows, hidden), h, 0))],)

        units = [piece(a, h) + (r, h) for r, a in ((0, dy_loc), (1, dy_mate)) for h in hs]
        dg, du = _mid_grads(place, units, wd_loc, ug4, uu4, 2, (), (zt,))
        x_own, dg = lax.optimization_barrier((x_loc, dg))
        x_half = [x_own[:rows], x_own[rows:]]
        dy_x[0], dy_y[1], dg, *x_half = lax.optimization_barrier((dy_x[0], dy_y[1], dg, *x_half))
        dy_d = [send(dy_x[0], 4), send(dy_y[1], 2)]
        keep_a, keep_b, give_a, give_b = _partials(
            dg, du, 2, wg_loc, wu_loc,
            [((0, 0), (1, 0)), ((0, 1), (1, 1)), ((2, 0), (3, 0)), ((2, 1), (3, 1))], [2, 2, 2, 2])
        mate_a, mate_b = send(give_a, 1), send(give_b, 1)
        *x_half, keep_a = lax.optimization_barrier((*x_half, keep_a))
        x_x, x_y = [send(a, 2) for a in x_half], [send(a, 4) for a in x_half]
        dy_x[1], dy_y[0], keep_a = lax.optimization_barrier((dy_x[1], dy_y[0], keep_a))
        dy_xm, dy_ym = [send(a, 1) for a in dy_x], [send(a, 1) for a in dy_y]
        zt = _z_transposed(place, ug4, uu4, 4, 4, zt, (keep_a, dy_x[1], dy_y[0]))

        near = ((2, dy_x), (3, dy_xm), (4, dy_y), (5, dy_ym))
        units = [piece(ps[h]) + (r, h) for r, ps in near for h in hs]
        dg, du = _mid_grads(place, units, wd_loc, ug4, uu4, 0, (dg, du), (zt, keep_a))
        dy_d = list(lax.optimization_barrier((*dy_d, dg))[:2])
        dy_dm = [send(a, 1) for a in dy_d]
        sides = ((0, 2), (1, 3), (6, 4), (7, 5))
        targets = [((a, h), (b, h)) for a, b in sides for h in hs]
        p = _partials(dg, du, 0, wg_loc, wu_loc, targets, [2] * 8)
        *xs, near_x, near_y, x_own = lax.optimization_barrier((*x_x, *x_y, p[0], p[4], x_own))
        x_x, x_y = xs[:2], xs[2:]
        x_d = [send(x_x[0], 4), send(x_y[1], 2)]
        x_mate, *xm = [send(a, 1) for a in (x_own, *x_x, *x_y)]
        near_x, near_y = send(near_x, 2), send(near_y, 4)
        pass_a, pass_b = [p[6], send(p[7], 1)], [p[2], send(p[3], 1)]

        units = [piece(a) + (r, h) for r, ps in ((6, dy_d), (7, dy_dm)) for h, a in enumerate(ps)]
        dg, du = _mid_grads(place, units, wd_loc, ug4, uu4, 3, (dg, du), (p[0],))
        targets = [((2 * k, h), (2 * k + 1, h)) for k in range(2) for h in hs]
        q = _partials(dg, du, 3, wg_loc, wu_loc, targets, [2] * 4)
        pass_a += [send(q[0], 2), send(q[2], 3)]
        pass_b += [send(q[1], 4), send(q[3], 5)]

        late_x, late_y, _ = lax.optimization_barrier((p[1], p[5], q[0]))
        done_a = [keep_a, mate_a, near_x, send(late_x, 3)]
        done_b = [keep_b, mate_b, near_y, send(late_y, 5)]

        x_d = list(lax.optimization_barrier((*x_d, q[0]))[:2])
        x_dm = [send(a, 1) for a in x_d]
        strip = 512

        def cols(a):
            return (a, _along((a.shape[0], strip), 1, 0, 0))

        dy_rows = [cols(a) for a in (dy_loc, dy_mate, *dy_x, *dy_xm, *dy_y, *dy_ym, *dy_d, *dy_dm)]
        grad_wd = _wdown(zt, dy_rows, (q[0],), strip)
        x_rows = [cols(a) for a in (*x_x, *xm[:2], *x_y, *xm[2:], x_loc, x_mate, *x_d, *x_dm)]
        grad_wg = _wcol(dg.reshape(-1, width), x_rows, (grad_wd,))
        far_a, far_b, last = [], [], (grad_wg,)
        for h in hs:
            away_a, away_b = _far_sums(pass_a, pass_b, h, last)
            far_a.append(send(away_a, 4))
            far_b.append(send(away_b, 2))
            last = (away_a,)
        grad_wu = _wcol(du.reshape(-1, width), x_rows, last)
        grad_x = _final_sums(done_a, done_b, far_a[0], far_b[0], 0, None, (grad_wu,))
        grad_x = _final_sums(done_a, done_b, far_a[1], far_b[1], 1, grad_x, ())
        return grad_x, grad_wg, grad_wu, grad_wd

    row_spec = P(('dp', 'tp'), None)
    col_spec = P(None, 'tp')
    part_cols = P('dp', 'tp')
    return jax.shard_map(layer, mesh=mesh,
                         in_specs=(row_spec, col_spec, col_spec, P('tp', None), part_cols, part_cols, row_spec),
                         out_specs=(row_spec, part_cols, part_cols, row_spec),
                         check_vma=False)
```

```python
import jax
import jax.numpy as jnp
from jax import lax
from jax.experimental import pallas as pl
from jax.experimental.pallas import tpu as pltpu
from jax.sharding import PartitionSpec as P


F32 = jnp.float32
BF16 = jnp.bfloat16
CHUNKS = 2
NT = (((1,), (1,)), ((), ()))
NN = (((1,), (0,)), ((), ()))
VMEM_LIMIT = 67_043_328


def _call(body, args, *, flops, nbytes, grid, in_specs, out_specs, out_shape, place=None, deps=(), aliases=None):
    n_in, n_dep, first = len(in_specs), len(deps), 0 if place is None else 1

    def kernel(*refs):
        body(*refs[first:first + n_in], *refs[first + n_in + n_dep:])

    return pl.pallas_call(
        kernel,
        grid_spec=pltpu.PrefetchScalarGridSpec(
            num_scalar_prefetch=first, grid=grid,
            in_specs=list(in_specs) + [pl.BlockSpec(memory_space=pl.ANY)] * n_dep, out_specs=out_specs),
        out_shape=out_shape,
        input_output_aliases=aliases or {},
        compiler_params=pltpu.CompilerParams(vmem_limit_bytes=VMEM_LIMIT),
        cost_estimate=pl.CostEstimate(flops=flops, bytes_accessed=nbytes, transcendentals=0),
    )(*([] if place is None else [place]), *args, *deps)


def _fixed(shape, *index):
    def at(i, *place):
        return tuple(place[0][int(e[1:])] if isinstance(e, str) else e for e in index)

    return pl.BlockSpec(shape, at, pipeline_mode=pl.Buffered(1))


def _along(shape, axis, *index, offset=0):
    def at(i, *place):
        out = [place[0][int(e[1:])] if isinstance(e, str) else e for e in index]
        out[axis] = i + offset
        return tuple(out)

    return pl.BlockSpec(shape, at)


def _value(ref):
    return ref[...].reshape(ref.shape[-2:]) if len(ref.shape) < 4 or ref.shape[1] == 1 else ref[...].reshape(-1, ref.shape[-1])


def _rows_of(refs):
    vals = [_value(r) for r in refs]
    return vals[0] if len(vals) == 1 else jnp.concatenate(vals, axis=0)


def _copy_body(in_ref, out_ref):
    out_ref[...] = in_ref[...]


def _copy_half(a, h, deps, step=64):
    tok, hidden = a.shape
    steps = tok // CHUNKS // step
    return _call(
        _copy_body, (a,), flops=tok * hidden, nbytes=2 * tok * hidden, deps=deps, grid=(steps,),
        in_specs=[_along((step, hidden), 0, 0, 0, offset=h * steps)], out_specs=_along((step, hidden), 0, 0, 0),
        out_shape=jax.ShapeDtypeStruct((tok // CHUNKS, hidden), a.dtype))


def _z_body(ug_ref, uu_ref, *rest):
    _, both, rows, width = ug_ref.shape
    gate = ug_ref[...].reshape(both * rows, width).astype(F32)
    z = gate * jax.nn.sigmoid(gate) * uu_ref[...].reshape(both * rows, width).astype(F32)
    rest[-1][...] = z.astype(BF16).T


def _z_transposed(place, ug4, uu4, first, count, old, deps):
    group, both, rows, width = ug4.shape
    tok = both * rows
    spec = pl.BlockSpec((1, both, rows, width), lambda i, p: (p[i + first], 0, 0, 0))
    args = [ug4, uu4] + ([] if old is None else [old])
    return _call(
        _z_body, args, flops=count * tok * width * 8, nbytes=count * tok * width * 6, place=place, deps=deps,
        grid=(count,), in_specs=[spec, spec] + [pl.BlockSpec(memory_space=pl.ANY)] * (len(args) - 2),
        out_specs=pl.BlockSpec((width, tok), lambda i, p: (0, i + first)),
        out_shape=jax.ShapeDtypeStruct((width, group * tok), BF16),
        aliases=None if old is None else {3: 0})


def _mid_grads(place, units, wd, ug4, uu4, lead, old, deps, step=256):
    width, hidden = wd.shape
    rows = ug4.shape[2]
    n = len(units)
    pieces = [p for ps, _, _ in units for p in ps]
    counts = [len(ps) for ps, _, _ in units]

    def body(*refs):
        dy_refs, refs = refs[:len(pieces)], refs[len(pieces):]
        wd_ref, ug_refs, uu_refs, (dg_ref, du_ref) = refs[0], refs[1:1 + n], refs[1 + n:1 + 2 * n], refs[-2:]
        at = 0
        for u in range(0, n, 2):
            take = counts[u] + counts[u + 1]
            dy = _rows_of(dy_refs[at:at + take])
            at += take
            g2 = lax.dot_general(dy, wd_ref[...], NT, preferred_element_type=F32)
            for k in range(2):
                g = g2[k * rows:(k + 1) * rows]
                gate = ug_refs[u + k][0, 0].astype(F32)
                up = uu_refs[u + k][0, 0].astype(F32)
                sig = jax.nn.sigmoid(gate)
                dg_ref[u + k] = (g * up * sig * (1.0 + gate * (1.0 - sig))).astype(BF16)
                du_ref[u + k] = (g * (gate * sig)).astype(BF16)

    u_specs = [_along((1, 1, rows, step), 3, f'r{r}', h, 0, 0) for _, r, h in units]
    o_spec = _along((n, rows, step), 2, lead, 0, 0)
    out = jax.ShapeDtypeStruct((ug4.shape[0] * ug4.shape[1], rows, width), BF16)
    args = [a for a, _ in pieces] + [wd] + [ug4] * n + [uu4] * n + list(old)
    return _call(
        body, args, place=place, deps=deps, aliases={len(args) - 1: 0, len(args): 1} if old else None,
        flops=2 * n * rows * hidden * width, nbytes=2 * (n * rows * (hidden + 4 * width) + width * hidden),
        grid=(width // step,),
        in_specs=[s for _, s in pieces] + [_along((step, hidden), 0, 0, 0)] + u_specs + u_specs
        + [pl.BlockSpec(memory_space=pl.ANY)] * len(old),
        out_specs=[o_spec, o_spec], out_shape=[out, out])


def _partials(dg3, du3, lead, wg, wu, targets, shapes, deps=(), step=256):
    n, (_, rows, width) = len(targets), dg3.shape
    hidden = wg.shape[0]
    half = hidden // 2

    def body(dg_ref, du_ref, wga_ref, wgb_ref, wua_ref, wub_ref, *outs):
        dg = dg_ref[...].reshape(n * rows, width)
        du = du_ref[...].reshape(n * rows, width)
        wg_t = jnp.concatenate([wga_ref[...], wgb_ref[...]], axis=0)
        wu_t = jnp.concatenate([wua_ref[...], wub_ref[...]], axis=0)
        acc = (lax.dot_general(dg, wg_t, NT, preferred_element_type=F32)
               + lax.dot_general(du, wu_t, NT, preferred_element_type=F32)).astype(BF16)
        for u, pair in enumerate(targets):
            for side, (o, lead) in enumerate(pair):
                outs[o][lead] = acc[u * rows:(u + 1) * rows, side * step:(side + 1) * step]

    tiles = half // step
    left, right = _along((step, width), 0, 0, 0), _along((step, width), 0, 0, 0, offset=tiles)
    return _call(
        body, (dg3, du3, wg, wg, wu, wu), deps=deps,
        flops=4 * n * rows * hidden * width, nbytes=2 * (n * rows * (hidden + 2 * width) + 2 * width * hidden),
        grid=(tiles,),
        in_specs=[_fixed((n, rows, width), lead, 0, 0)] * 2 + [left, right, left, right],
        out_specs=[_along((m, rows, step), 2, 0, 0, 0) for m in shapes],
        out_shape=[jax.ShapeDtypeStruct((m, rows, half), BF16) for m in shapes])


def _wdown(zt, pieces, deps, step=512):
    width, tok = zt.shape
    hidden = pieces[0][0].shape[-1]

    def body(zt_ref, *refs):
        refs[-1][...] = lax.dot_general(zt_ref[...], _rows_of(refs[:-1]), NN, preferred_element_type=F32)

    return _call(
        body, [zt] + [a for a, _ in pieces], deps=deps,
        flops=2 * tok * width * hidden, nbytes=2 * tok * (width + hidden) + 4 * width * hidden,
        grid=(hidden // step,), in_specs=[_fixed(zt.shape, 0, 0)] + [s for _, s in pieces],
        out_specs=_along((width, step), 1, 0, 0),
        out_shape=jax.ShapeDtypeStruct((width, hidden), F32))


def _wcol(d_rows, pieces, deps, step=512):
    tok, width = d_rows.shape
    hidden = pieces[0][0].shape[-1]

    def body(d_ref, *refs):
        xt = _rows_of(refs[:-1]).T
        refs[-1][...] = lax.dot_general(xt, d_ref[...], NN, preferred_element_type=F32)

    return _call(
        body, [d_rows] + [a for a, _ in pieces], deps=deps,
        flops=2 * tok * width * hidden, nbytes=2 * tok * (width + hidden) + 4 * width * hidden,
        grid=(hidden // step,), in_specs=[_fixed(d_rows.shape, 0, 0)] + [s for _, s in pieces],
        out_specs=_along((step, width), 0, 0, 0),
        out_shape=jax.ShapeDtypeStruct((hidden, width), F32))


def _sum(refs):
    total = refs[0][...].astype(F32)
    for r in refs[1:]:
        total = total + r[...].astype(F32)
    return total


def _far_sums(terms_a, terms_b, chunk, deps, step=512):
    _, rows, half = terms_a[0].shape
    n = len(terms_a)

    def body(*refs):
        refs[2 * n][...] = _sum(refs[:n])[0]
        refs[2 * n + 1][...] = _sum(refs[n:2 * n])[0]

    return _call(
        body, [*terms_a, *terms_b], flops=8 * rows * half, nbytes=24 * rows * half, deps=deps,
        grid=(half // step,), in_specs=[_along((1, rows, step), 2, chunk, 0, 0)] * (2 * n),
        out_specs=[_along((rows, step), 1, 0, 0)] * 2, out_shape=[jax.ShapeDtypeStruct((rows, half), F32)] * 2)


def _final_sums(terms_a, terms_b, far_a, far_b, chunk, whole, deps, step=64):
    rows, half = far_a.shape
    n = len(terms_a)
    steps = rows // step
    old = [] if whole is None else [whole]

    def body(*refs):
        o_ref = refs[-1]
        o_ref[:, :half] = (_sum(refs[:n])[0] + refs[2 * n][...]).astype(BF16)
        o_ref[:, half:] = (_sum(refs[n:2 * n])[0] + refs[2 * n + 1][...]).astype(BF16)

    args = [*terms_a, *terms_b, far_a, far_b] + old
    return _call(
        body, args, flops=8 * rows * half, nbytes=28 * rows * half, deps=deps, grid=(steps,),
        in_specs=[_along((1, step, half), 1, chunk, 0, 0)] * (2 * n)
        + [_along((step, half), 0, 0, 0)] * 2 + [pl.BlockSpec(memory_space=pl.ANY)] * len(old),
        out_specs=_along((step, 2 * half), 0, 0, 0, offset=chunk * steps),
        out_shape=jax.ShapeDtypeStruct((CHUNKS * rows, 2 * half), BF16),
        aliases={len(args) - 1: 0} if old else None)


def solution(mesh):
    group = mesh.shape['tp']

    def send(value, away):
        return lax.ppermute(value, 'tp', [(d, d ^ away) for d in range(group)])


    def layer(x_loc, wg_loc, wu_loc, wd_loc, ug_loc, uu_loc, dy_loc):
        tok, hidden = x_loc.shape
        width = wd_loc.shape[0]
        rows = tok // CHUNKS
        place = lax.axis_index('tp').astype(jnp.int32) ^ jnp.arange(group, dtype=jnp.int32)
        ug4 = ug_loc.reshape(group, CHUNKS, rows, width)
        uu4 = uu_loc.reshape(group, CHUNKS, rows, width)
        hs = range(CHUNKS)

        dy_mate = send(dy_loc, 1)
        first = _copy_half(dy_loc, 0, ())
        halves = [first, _copy_half(dy_loc, 1, (first,))]
        dy_x, dy_y = [None, None], [None, None]
        for h in hs:
            dy_x[h] = send(halves[h], 2)
            dy_y[1 - h] = send(halves[1 - h], 4)
        zt = _z_transposed(place, ug4, uu4, 0, 4, None, ())

        def piece(a, h=0):
            return ([(a, _fixed((rows, hidden), h, 0))],)

        units = [piece(a, h) + (r, h) for r, a in ((0, dy_loc), (1, dy_mate)) for h in hs]
        dg, du = _mid_grads(place, units, wd_loc, ug4, uu4, 2, (), (zt,))
        x_own, dg = lax.optimization_barrier((x_loc, dg))
        x_half = [x_own[:rows], x_own[rows:]]
        dy_x[0], dy_y[1], dg, *x_half = lax.optimization_barrier((dy_x[0], dy_y[1], dg, *x_half))
        dy_d = [send(dy_x[0], 4), send(dy_y[1], 2)]
        keep_a, keep_b, give_a, give_b = _partials(
            dg, du, 2, wg_loc, wu_loc,
            [((0, 0), (1, 0)), ((0, 1), (1, 1)), ((2, 0), (3, 0)), ((2, 1), (3, 1))], [2, 2, 2, 2])
        mate_a, mate_b = send(give_a, 1), send(give_b, 1)
        *x_half, keep_a = lax.optimization_barrier((*x_half, keep_a))
        x_x, x_y = [send(a, 2) for a in x_half], [send(a, 4) for a in x_half]
        dy_x[1], dy_y[0], keep_a = lax.optimization_barrier((dy_x[1], dy_y[0], keep_a))
        dy_xm, dy_ym = [send(a, 1) for a in dy_x], [send(a, 1) for a in dy_y]
        zt = _z_transposed(place, ug4, uu4, 4, 4, zt, (keep_a, dy_x[1], dy_y[0]))

        near = ((2, dy_x), (3, dy_xm), (4, dy_y), (5, dy_ym))
        units = [piece(ps[h]) + (r, h) for r, ps in near for h in hs]
        dg, du = _mid_grads(place, units, wd_loc, ug4, uu4, 0, (dg, du), (zt, keep_a))
        dy_d = list(lax.optimization_barrier((*dy_d, dg))[:2])
        dy_dm = [send(a, 1) for a in dy_d]
        sides = ((0, 2), (1, 3), (6, 4), (7, 5))
        targets = [((a, h), (b, h)) for a, b in sides for h in hs]
        p = _partials(dg, du, 0, wg_loc, wu_loc, targets, [2] * 8)
        *xs, near_x, near_y, x_own = lax.optimization_barrier((*x_x, *x_y, p[0], p[4], x_own))
        x_x, x_y = xs[:2], xs[2:]
        x_d = [send(x_x[0], 4), send(x_y[1], 2)]
        x_mate, *xm = [send(a, 1) for a in (x_own, *x_x, *x_y)]
        near_x, near_y = send(near_x, 2), send(near_y, 4)
        pass_a, pass_b = [p[6], send(p[7], 1)], [p[2], send(p[3], 1)]

        units = [piece(a) + (r, h) for r, ps in ((6, dy_d), (7, dy_dm)) for h, a in enumerate(ps)]
        dg, du = _mid_grads(place, units, wd_loc, ug4, uu4, 3, (dg, du), (p[0],))
        targets = [((2 * k, h), (2 * k + 1, h)) for k in range(2) for h in hs]
        q = _partials(dg, du, 3, wg_loc, wu_loc, targets, [2] * 4)
        pass_a += [send(q[0], 2), send(q[2], 3)]
        pass_b += [send(q[1], 4), send(q[3], 5)]

        late_x, late_y, _ = lax.optimization_barrier((p[1], p[5], q[0]))
        done_a = [keep_a, mate_a, near_x, send(late_x, 3)]
        done_b = [keep_b, mate_b, near_y, send(late_y, 5)]

        x_d = list(lax.optimization_barrier((*x_d, q[0]))[:2])
        x_dm = [send(a, 1) for a in x_d]
        strip = 512

        def cols(a):
            return (a, _along((a.shape[0], strip), 1, 0, 0))

        dy_rows = [cols(a) for a in (dy_loc, dy_mate, *dy_x, *dy_xm, *dy_y, *dy_ym, *dy_d, *dy_dm)]
        grad_wd = _wdown(zt, dy_rows, (q[0],), strip)
        x_rows = [cols(a) for a in (*x_x, *xm[:2], *x_y, *xm[2:], x_loc, x_mate, *x_d, *x_dm)]
        grad_wg = _wcol(dg.reshape(-1, width), x_rows, (grad_wd,))
        far_a, far_b, last = [], [], (grad_wg,)
        for h in hs:
            away_a, away_b = _far_sums(pass_a, pass_b, h, last)
            far_a.append(send(away_a, 4))
            far_b.append(send(away_b, 2))
            last = (away_a,)
        grad_wu = _wcol(du.reshape(-1, width), x_rows, last)
        grad_x = _final_sums(done_a, done_b, far_a[0], far_b[0], 0, None, (grad_wu,))
        grad_x = _final_sums(done_a, done_b, far_a[1], far_b[1], 1, grad_x, ())
        return grad_x, grad_wg, grad_wu, grad_wd

    row_spec = P(('dp', 'tp'), None)
    col_spec = P(None, 'tp')
    part_cols = P('dp', 'tp')
    return jax.shard_map(layer, mesh=mesh,
                         in_specs=(row_spec, col_spec, col_spec, P('tp', None), part_cols, part_cols, row_spec),
                         out_specs=(row_spec, part_cols, part_cols, row_spec),
                         check_vma=False)
```
